128 devices in a mesh: mix: 4 (over z), span: 32 (over x, y, core).
Axes of the slice: x: 4, y: 4, z: 4, core: 2. Of those that a mesh axis runs over, the one named last changes fastest.
Arguments:
- mixture: bfloat16 [2048, 256, 256], P(('mix', 'span')), parts along dimension 0, may hold values from -16 to 16, as said below
- w_query: bfloat16 [2, 256, 256], replicated, may hold values from -4 to 4
- w_key: bfloat16 [2, 256, 256], replicated, may hold values from -4 to 4
- w_value: bfloat16 [2, 256, 256], replicated, may hold values from -0.375 to 0.375
- w_out: bfloat16 [2, 256, 256], replicated, may hold values from -0.375 to 0.375
- w_up: bfloat16 [2, 256, 1024], replicated, may hold values from -0.375 to 0.375
- w_down: bfloat16 [2, 1024, 256], replicated, may hold values from -0.1875 to 0.1875
- ln_gain: float32 [2, 2, 256], replicated, may hold values from 0.25 to 1.75
- gln_gain: float32 [2, 256], replicated, may hold values from 0.25 to 1.75
- gln_bias: float32 [2, 256], replicated, may hold values from -3 to 3
Outputs:
- block_out: bfloat16 [2048, 256, 256], P(('mix', 'span')), parts along dimension 0
The draws below stay inside these ranges and needn't reach their ends.
There are 4 independent parts, one for each index of `mix`. The reference program is written for one: setup_inputs(seed, part) draws one part's arguments, and reference() takes and returns one part's arrays. A program takes and returns all parts, laid end to end along the dimension named above; an argument that names none is the same for every part. Nothing has to cross between parts.
Inputs may be any that keep to these rules, and one draw needn't show every extreme that they name: `mixture`: entries of order one, scaled by a factor per segment.
All inputs are finite; a program needn't handle non-finite values.
Results may differ from the reference program's by a relative error of at most 0.0057.
Values may be sent and summed in bfloat16 or wider, within the bound.
No kernel may reach another device: no remote copies, remote signals or barrier semaphores. Data moves between devices by JAX's collectives and lax.ppermute only.
A program may use at most 128 MiB of HBM per device.

```python
import math
import jax
import jax.numpy as jnp
from jax import lax

D = 256
HEADS = 8
FF = 1024
FRAMES = 256
SEGMENTS = 512


def draw_mixture(key, part):
    keys = jax.random.split(key, 4)
    scales = jnp.exp(jax.random.uniform(keys[0], (SEGMENTS, 1, 1), jnp.float32, math.log(0.25), math.log(4.0)))
    offsets = 0.5 * jax.random.normal(keys[1], (SEGMENTS, 1, 1), jnp.float32)
    result = offsets + scales * jax.random.normal(keys[2], (SEGMENTS, FRAMES, D), jnp.float32)
    return jnp.clip(result, -16.0, 16.0).astype(jnp.bfloat16)


def query_key_pair(key):
    base = jax.random.normal(jax.random.fold_in(key, 11), (2, D, D), jnp.float32) * D ** (-0.5)
    other = jax.random.normal(jax.random.fold_in(key, 12), (2, D, D), jnp.float32) * D ** (-0.5)
    return (jnp.clip(base, -4.0, 4.0), jnp.clip(other, -4.0, 4.0))


def draw_w_query(key, part):
    return query_key_pair(key)[0].astype(jnp.bfloat16)


def draw_w_key(key, part):
    return query_key_pair(key)[1].astype(jnp.bfloat16)


def normal_values(rng, dims, scale, reach, kind=jnp.bfloat16):
    entries = scale * jax.random.normal(rng, dims, jnp.float32)
    return jnp.clip(entries, min=-reach, max=reach).astype(kind)


def setup_inputs(seed: int = 0, part: int = 0) -> dict:
    arg_keys = jax.random.split(jax.random.key(seed), 11)
    own_keys = jax.random.split(jax.random.fold_in(arg_keys[10], part), 11)
    mixture = draw_mixture(jax.random.fold_in(jax.random.fold_in(arg_keys[10], part), 71), part)
    w_query = draw_w_query(jax.random.fold_in(arg_keys[10], 71), part)
    w_key = draw_w_key(jax.random.fold_in(arg_keys[10], 71), part)
    w_value = normal_values(arg_keys[3], (2, D, D), D ** -0.5, 0.375)
    w_out = normal_values(arg_keys[4], (2, D, D), D ** -0.5, 0.375)
    w_up = normal_values(arg_keys[5], (2, D, FF), D ** -0.5, 0.375)
    w_down = normal_values(arg_keys[6], (2, FF, D), FF ** -0.5, 0.1875)
    ln_gain = jnp.clip(1.0 + 0.15 * jax.random.normal(arg_keys[7], (2, 2, D), jnp.float32), 0.25, 1.75)
    gln_gain = jnp.clip(1.0 + 0.15 * jax.random.normal(arg_keys[8], (2, D), jnp.float32), 0.25, 1.75)
    gln_bias = normal_values(arg_keys[9], (2, D), 0.5, 3.0, jnp.float32)
    return {"mixture": mixture, "w_query": w_query, "w_key": w_key, "w_value": w_value, "w_out": w_out, "w_up": w_up, "w_down": w_down, "ln_gain": ln_gain, "gln_gain": gln_gain, "gln_bias": gln_bias}


norm_eps = 1e-05

def pos_table(length, width):
    places = jnp.arange(length, dtype=jnp.float32)[:, None]
    column = jnp.arange(width)
    rates = jnp.exp(-(2 * (column // 2)).astype(jnp.float32) / width * math.log(10000.0))
    angles = places * rates[None, :]
    return jnp.where((column % 2 == 0)[None, :], jnp.sin(angles), jnp.cos(angles))

def norm_rows(rows, gain):
    center = lax.optimization_barrier(jnp.mean(rows, axis=-1, keepdims=True))
    shifted = rows - center
    spread = lax.optimization_barrier(jnp.mean(shifted * shifted, axis=-1, keepdims=True))
    return shifted * lax.rsqrt(spread + norm_eps) * gain

def attend(queries, key_rows, values):
    length = queries.shape[0]
    split_q = queries.reshape(length, HEADS, D // HEADS).astype(jnp.float32)
    split_k = key_rows.reshape(length, HEADS, D // HEADS).astype(jnp.float32)
    split_v = values.reshape(length, HEADS, D // HEADS).astype(jnp.float32)
    scores = jnp.einsum('qhd,khd->hqk', split_q, split_k) / math.sqrt(D // HEADS)
    weights = jax.nn.softmax(scores, axis=-1).astype(jnp.bfloat16)
    context = jnp.einsum('hqk,khd->qhd', weights.astype(jnp.float32), split_v)
    return context.astype(jnp.bfloat16).reshape(length, D)

def encoder_layer(sequence, level, w_query, w_key, w_value, w_out, w_up, w_down, ln_gain):
    length = sequence.shape[0]
    inputs = sequence.astype(jnp.float32) + pos_table(length, D)
    normed = norm_rows(inputs, ln_gain[level, 0]).astype(jnp.bfloat16)
    queries = jnp.dot(normed, w_query[level], preferred_element_type=jnp.float32).astype(jnp.bfloat16)
    key_rows = jnp.dot(normed, w_key[level], preferred_element_type=jnp.float32).astype(jnp.bfloat16)
    values = jnp.dot(normed, w_value[level], preferred_element_type=jnp.float32).astype(jnp.bfloat16)
    context = attend(queries, key_rows, values)
    after_attn = inputs + jnp.dot(context, w_out[level], preferred_element_type=jnp.float32)
    normed_two = norm_rows(after_attn, ln_gain[level, 1]).astype(jnp.bfloat16)
    hidden = jax.nn.relu(jnp.dot(normed_two, w_up[level], preferred_element_type=jnp.float32)).astype(jnp.bfloat16)
    return after_attn + jnp.dot(hidden, w_down[level], preferred_element_type=jnp.float32)

def global_norm(rows, gain, bias):
    center = jnp.mean(rows)
    shifted = rows - center
    spread = jnp.mean(shifted * shifted)
    return gain * shifted * lax.rsqrt(spread + norm_eps) + bias

def reference(mixture, w_query, w_key, w_value, w_out, w_up, w_down, ln_gain, gln_gain, gln_bias):

    def intra_one(block_rows):
        return encoder_layer(block_rows, 0, w_query, w_key, w_value, w_out, w_up, w_down, ln_gain)

    def inter_one(sequence):
        return encoder_layer(sequence, 1, w_query, w_key, w_value, w_out, w_up, w_down, ln_gain)
    intra = lax.map(intra_one, mixture)
    intra_out = (global_norm(intra, gln_gain[0], gln_bias[0]) + mixture.astype(jnp.float32)).astype(jnp.bfloat16)
    across = jnp.transpose(intra_out, (1, 0, 2))
    inter = lax.map(inter_one, across)
    final = (global_norm(inter, gln_gain[1], gln_bias[1]) + across.astype(jnp.float32)).astype(jnp.bfloat16)
    return jnp.transpose(final, (1, 0, 2))
```

```python
import functools
import math

import jax
import jax.numpy as jnp
from jax import lax
from jax.experimental import pallas as pl
from jax.experimental.pallas import tpu as pltpu
from jax.sharding import PartitionSpec as P

D = 256
HEADS = 8
HD = D // HEADS
FF = 1024
EPS = 1e-05
AUG = HD + 16
F32 = jnp.float32
BF16 = jnp.bfloat16


def pos_table_t(length):
    places = jnp.arange(length, dtype=F32)[None, :]
    column = jnp.arange(D)
    rates = jnp.exp(-(2 * (column // 2)).astype(F32) / D * math.log(10000.0))
    angles = places * rates[:, None]
    return jnp.where((column % 2 == 0)[:, None], jnp.sin(angles), jnp.cos(angles))


def dot(a, b):
    return lax.dot_general(a, b, (((1,), (0,)), ((), ())), preferred_element_type=F32)


def norm_cols(x, gain):
    center = jnp.mean(x, axis=0, keepdims=True)
    shifted = x - center
    spread = jnp.mean(shifted * shifted, axis=0, keepdims=True)
    return shifted * lax.rsqrt(spread + EPS) * gain


def layer_body(xt, g1, g2, wq_t, w_k, wv_t, wo_t, wup_t, wdn_t, vaug, ctx):
    length = xt.shape[1]
    chunk = 256
    normed = norm_cols(xt, g1).astype(BF16)
    scale = math.log2(math.e) / math.sqrt(HD)
    q_t = (dot(wq_t, normed) * scale).astype(BF16)
    v_t = dot(wv_t, normed).astype(BF16)
    keys = dot(normed.T, w_k).astype(BF16)
    for h in range(HEADS):
        vaug[h * AUG : h * AUG + HD, :] = v_t[h * HD : (h + 1) * HD, :]
    for c in range(length // chunk):
        lanes = slice(c * chunk, (c + 1) * chunk)
        for h in range(HEADS):
            block, at = divmod(h * HD, 128)
            parts = []
            if at:
                parts.append(jnp.zeros((at, chunk), BF16))
            parts.append(q_t[h * HD : (h + 1) * HD, lanes])
            if at + HD < 128:
                parts.append(jnp.zeros((128 - at - HD, chunk), BF16))
            q_pad = jnp.concatenate(parts, axis=0)
            scores = dot(keys[:, block * 128 : (block + 1) * 128], q_pad)
            top = jnp.max(scores, axis=0, keepdims=True)
            weights = jnp.exp2(scores - top).astype(BF16)
            mixed = dot(vaug[h * AUG : (h + 1) * AUG, :], weights)
            ctx[h * HD : (h + 1) * HD, lanes] = (
                mixed[:HD, :] * (1.0 / mixed[HD : HD + 1, :])
            ).astype(BF16)
    after = xt + dot(wo_t, ctx[...])
    normed_two = norm_cols(after, g2).astype(BF16)
    hidden = jnp.maximum(dot(wup_t, normed_two), 0.0).astype(BF16)
    return after + dot(wdn_t, hidden)


def layer_kernel(x_ref, pos_ref, g1_ref, g2_ref, wq_ref, wk_ref, wv_ref, wo_ref, wup_ref, wdn_ref,
                 y_ref, stat_ref, wq_t, wv_t, wo_t, wup_t, wdn_t, vaug, ctx):
    length = pos_ref.shape[1]

    @pl.when(pl.program_id(0) == 0)
    def _():
        wq_t[...] = wq_ref[...].T
        wv_t[...] = wv_ref[...].T
        wo_t[...] = wo_ref[...].T
        wup_t[...] = wup_ref[...].T
        wdn_t[...] = wdn_ref[...].T
        vaug[...] = jnp.ones_like(vaug)
        stat_ref[...] = jnp.zeros_like(stat_ref)

    x = x_ref[...].reshape(length, D)
    xt = x.T.astype(F32) + pos_ref[...]
    y_t = layer_body(xt, g1_ref[...], g2_ref[...], wq_t[...], wk_ref[...], wv_t[...], wo_t[...],
                     wup_t[...], wdn_t[...], vaug, ctx)
    part = y_t.reshape(D // 8, 8, length)
    stat_ref[0] += jnp.sum(part, axis=0)
    stat_ref[1] += jnp.sum(part * part, axis=0)
    y_ref[...] = y_t.astype(BF16).T.reshape(y_ref.shape)


def layer(x, steps, x_block, x_map, length, pos, g1, g2, w_q, w_k, w_v, w_o, w_u, w_d, name):
    whole = lambda a: pl.BlockSpec(a.shape, lambda i: (0,) * a.ndim)
    consts = (pos, g1, g2, w_q, w_k, w_v, w_o, w_u, w_d)
    return pl.pallas_call(
        layer_kernel,
        grid=(steps,),
        in_specs=[pl.BlockSpec(x_block, x_map)] + [whole(a) for a in consts],
        out_specs=[pl.BlockSpec(x_block, x_map), pl.BlockSpec((2, 8, length), lambda i: (0, 0, 0))],
        out_shape=[jax.ShapeDtypeStruct(x.shape, BF16), jax.ShapeDtypeStruct((2, 8, length), F32)],
        scratch_shapes=[
            pltpu.VMEM((D, D), BF16), pltpu.VMEM((D, D), BF16), pltpu.VMEM((D, D), BF16),
            pltpu.VMEM((FF, D), BF16), pltpu.VMEM((D, FF), BF16),
            pltpu.VMEM((HEADS * AUG, length), BF16), pltpu.VMEM((D, length), BF16),
        ],
        compiler_params=pltpu.CompilerParams(dimension_semantics=("arbitrary",)),
        name=name,
    )(x, *consts)


def shared_stats(stat, cells):
    mine = jnp.sum(stat, axis=(1, 2))
    copies = jnp.broadcast_to(mine[None, None, :], (lax.axis_size("span"), 1, 2))
    total = lax.all_to_all(copies, "span", split_axis=0, concat_axis=0, tiled=True).sum(axis=(0, 1))
    center = total[0] / cells
    spread = total[1] / cells - center * center
    return center, lax.rsqrt(spread + EPS)


def body(mixture, w_query, w_key, w_value, w_out, w_up, w_down, ln_gain, gln_gain, gln_bias):
    shards = lax.axis_size("span")
    segs, frames, _ = mixture.shape
    own = frames // shards
    total = segs * shards
    cells = float(total * frames * D)
    weights = lambda l: (w_query[l], w_key[l], w_value[l], w_out[l], w_up[l], w_down[l])
    gains = lambda l: (ln_gain[l, 0][:, None], ln_gain[l, 1][:, None])

    intra, stat = layer(mixture, segs, (1, frames, D), lambda i: (i, 0, 0), frames,
                        pos_table_t(frames), *gains(0), *weights(0), name="intra")
    center, inv = shared_stats(stat, cells)
    intra_out = (gln_gain[0] * (intra.astype(F32) - center) * inv + gln_bias[0]
                 + mixture.astype(F32)).astype(BF16)
    by_frame = jnp.swapaxes(intra_out, 0, 1).reshape(shards, own, segs, D)
    moved = lax.all_to_all(by_frame, "span", split_axis=0, concat_axis=0, tiled=True)

    inter, stat = layer(moved, own, (shards, 1, segs, D), lambda i: (0, i, 0, 0), total,
                        pos_table_t(total), *gains(1), *weights(1), name="inter")
    center, inv = shared_stats(stat, cells)
    back = lax.all_to_all(inter, "span", split_axis=0, concat_axis=0, tiled=True)
    back = back.reshape(frames, segs, D)
    final = (gln_gain[1] * (back.astype(F32) - center) * inv + gln_bias[1]
             + jnp.swapaxes(intra_out, 0, 1).astype(F32)).astype(BF16)
    return jnp.swapaxes(final, 0, 1)


def solution(mesh):
    in_specs = (P(("mix", "span"), None, None), P(), P(), P(), P(), P(), P(), P(), P(), P())
    out_specs = P(("mix", "span"), None, None)
    return jax.shard_map(body, mesh=mesh, in_specs=in_specs, out_specs=out_specs, check_vma=False)
```

```python
import functools
import math

import jax
import jax.numpy as jnp
from jax import lax
from jax.experimental import pallas as pl
from jax.experimental.pallas import tpu as pltpu
from jax.sharding import PartitionSpec as P

D = 256
HEADS = 8
HD = D // HEADS
FF = 1024
EPS = 1e-05
AUG = HD + 16
F32 = jnp.float32
BF16 = jnp.bfloat16


def pos_table_t(length):
    places = jnp.arange(length, dtype=F32)[None, :]
    column = jnp.arange(D)
    rates = jnp.exp(-(2 * (column // 2)).astype(F32) / D * math.log(10000.0))
    angles = places * rates[:, None]
    return jnp.where((column % 2 == 0)[:, None], jnp.sin(angles), jnp.cos(angles))


def dot(a, b):
    return lax.dot_general(a, b, (((1,), (0,)), ((), ())), preferred_element_type=F32)


def norm_cols(x, gain):
    center = jnp.mean(x, axis=0, keepdims=True)
    shifted = x - center
    spread = jnp.mean(shifted * shifted, axis=0, keepdims=True)
    return shifted * lax.rsqrt(spread + EPS) * gain


CHUNK = 256


def phase_a(x, pos, g1, wq_t, wv_t, w_k, x_res, q_t, keys, vaug):
    xt = x.T.astype(F32) + pos
    x_res[...] = xt
    normed = norm_cols(xt, g1).astype(BF16)
    keys[...] = dot(normed.T, w_k).astype(BF16)
    scale = math.log2(math.e) / math.sqrt(HD)
    q_t[...] = (dot(wq_t, normed) * scale).astype(BF16)
    v_t = dot(wv_t, normed).astype(BF16)
    for h in range(HEADS):
        vaug[h * AUG : h * AUG + HD, :] = v_t[h * HD : (h + 1) * HD, :]


def phase_b(x_res, q_t, keys, vaug, wo_t, after, scores, weights, ctx):
    units = [(c, h) for c in range(q_t.shape[1] // CHUNK) for h in range(HEADS)]
    tops = {}

    def score(u):
        c, h = units[u]
        block, at = divmod(h * HD, 128)
        parts = []
        if at:
            parts.append(jnp.zeros((at, CHUNK), BF16))
        parts.append(q_t[h * HD : (h + 1) * HD, c * CHUNK : (c + 1) * CHUNK])
        if at + HD < 128:
            parts.append(jnp.zeros((128 - at - HD, CHUNK), BF16))
        s = dot(keys[:, block * 128 : (block + 1) * 128], jnp.concatenate(parts, axis=0))
        tops[u] = jnp.max(s, axis=0, keepdims=True)
        scores[u % len(scores)][...] = s

    def soften(u):
        s = scores[u % len(scores)][...]
        weights[u % len(weights)][...] = jnp.exp2(s - tops.pop(u)).astype(BF16)

    def mix(u):
        c, h = units[u]
        mixed = dot(vaug[h * AUG : (h + 1) * AUG, :], weights[u % len(weights)][...])
        ctx[h * HD : (h + 1) * HD, c * CHUNK : (c + 1) * CHUNK] = (
            mixed[:HD, :] * (1.0 / mixed[HD : HD + 1, :])
        ).astype(BF16)

    n = len(units)
    for u in range(n + 2):
        if u < n:
            score(u)
        if 0 <= u - 1 < n:
            soften(u - 1)
        if 0 <= u - 2 < n:
            mix(u - 2)
    after[...] = x_res[...] + dot(wo_t, ctx[...])


def phase_c(after, g2, wup_t, wdn_t, y_ref, stat_ref):
    aft = after[...]
    normed_two = norm_cols(aft, g2).astype(BF16)
    hidden = jnp.maximum(dot(wup_t, normed_two), 0.0).astype(BF16)
    y_t = aft + dot(wdn_t, hidden)
    part = y_t.reshape(D // 8, 8, y_t.shape[1])
    stat_ref[0] += jnp.sum(part, axis=0)
    stat_ref[1] += jnp.sum(part * part, axis=0)
    y_ref[...] = y_t.astype(BF16).T.reshape(y_ref.shape)


def layer_kernel(pair, x_ref, pos_ref, g1_ref, g2_ref, wq_ref, wk_ref, wv_ref, wo_ref, wup_ref, wdn_ref,
                 y_ref, stat_ref, wq_t, wv_t, wo_t, wup_t, wdn_t, *bufs):
    length = pos_ref.shape[1]
    slots = (bufs[0:5], bufs[5:10])
    ctx, scores, weights = bufs[10], bufs[11:14], bufs[14:17]
    step, last = pl.program_id(0), pl.num_programs(0) - 1

    def run(sub, a, b, c):
        here, other = slots[sub], slots[1 - sub]
        if c:
            phase_c(here[4], g2_ref[...], wup_t[...], wdn_t[...], pair(y_ref, sub), stat_ref)
        if a:
            phase_a(pair(x_ref, sub)[...].reshape(length, D), pos_ref[...], g1_ref[...], wq_t[...], wv_t[...],
                    wk_ref[...], *here[:4])
        if b:
            phase_b(*other[:4], wo_t[...], other[4], scores, weights, ctx)

    @pl.when(step == 0)
    def _():
        wq_t[...] = wq_ref[...].T
        wv_t[...] = wv_ref[...].T
        wo_t[...] = wo_ref[...].T
        wup_t[...] = wup_ref[...].T
        wdn_t[...] = wdn_ref[...].T
        for slot in slots:
            slot[3][...] = jnp.ones_like(slot[3])
        stat_ref[...] = jnp.zeros_like(stat_ref)
        run(0, True, False, False)
        run(1, True, True, False)

    @pl.when((step > 0) & (step < last))
    def _():
        run(0, True, True, True)
        run(1, True, True, True)

    @pl.when(step == last)
    def _():
        run(0, False, True, True)
        run(1, False, False, True)


def layer(x, count, x_block, x_map, pair, length, pos, g1, g2, w_q, w_k, w_v, w_o, w_u, w_d, name):
    whole = lambda a: pl.BlockSpec(a.shape, lambda i: (0,) * a.ndim)
    consts = (pos, g1, g2, w_q, w_k, w_v, w_o, w_u, w_d)
    pairs = count // 2
    slot = [
        pltpu.VMEM((D, length), F32), pltpu.VMEM((D, length), BF16), pltpu.VMEM((length, D), BF16),
        pltpu.VMEM((HEADS * AUG, length), BF16), pltpu.VMEM((D, length), F32),
    ]
    return pl.pallas_call(
        functools.partial(layer_kernel, pair),
        grid=(pairs + 1,),
        in_specs=[pl.BlockSpec(x_block, lambda i: x_map(jnp.minimum(i, pairs - 1)))] + [whole(a) for a in consts],
        out_specs=[pl.BlockSpec(x_block, lambda i: x_map(jnp.maximum(i - 1, 0))),
                   pl.BlockSpec((2, 8, length), lambda i: (0, 0, 0))],
        out_shape=[jax.ShapeDtypeStruct(x.shape, BF16), jax.ShapeDtypeStruct((2, 8, length), F32)],
        scratch_shapes=[
            pltpu.VMEM((D, D), BF16), pltpu.VMEM((D, D), BF16), pltpu.VMEM((D, D), BF16),
            pltpu.VMEM((FF, D), BF16), pltpu.VMEM((D, FF), BF16), *slot, *slot,
            pltpu.VMEM((D, length), BF16),
            *[pltpu.VMEM((length, CHUNK), F32)] * 3, *[pltpu.VMEM((length, CHUNK), BF16)] * 3,
        ],
        compiler_params=pltpu.CompilerParams(dimension_semantics=("arbitrary",)),
        name=name,
    )(x, *consts)


def shared_stats(stat, cells):
    mine = jnp.sum(stat, axis=(1, 2))
    copies = jnp.broadcast_to(mine[None, None, :], (lax.axis_size("span"), 1, 2))
    total = lax.all_to_all(copies, "span", split_axis=0, concat_axis=0, tiled=True).sum(axis=(0, 1))
    center = total[0] / cells
    spread = total[1] / cells - center * center
    return center, lax.rsqrt(spread + EPS)


def body(mixture, w_query, w_key, w_value, w_out, w_up, w_down, ln_gain, gln_gain, gln_bias):
    shards = lax.axis_size("span")
    segs, frames, _ = mixture.shape
    own = frames // shards
    total = segs * shards
    cells = float(total * frames * D)
    weights = lambda l: (w_query[l], w_key[l], w_value[l], w_out[l], w_up[l], w_down[l])
    gains = lambda l: (ln_gain[l, 0][:, None], ln_gain[l, 1][:, None])

    intra, stat = layer(mixture, segs, (2, frames, D), lambda i: (i, 0, 0), lambda r, k: r.at[k], frames,
                        pos_table_t(frames), *gains(0), *weights(0), name="intra")
    center, inv = shared_stats(stat, cells)
    intra_out = (gln_gain[0] * (intra.astype(F32) - center) * inv + gln_bias[0]
                 + mixture.astype(F32)).astype(BF16)
    by_frame = jnp.swapaxes(intra_out, 0, 1).reshape(shards, own, segs, D)
    moved = lax.all_to_all(by_frame, "span", split_axis=0, concat_axis=0, tiled=True)

    inter, stat = layer(moved, own, (shards, 2, segs, D), lambda i: (0, i, 0, 0), lambda r, k: r.at[:, k], total,
                        pos_table_t(total), *gains(1), *weights(1), name="inter")
    center, inv = shared_stats(stat, cells)
    back = lax.all_to_all(inter, "span", split_axis=0, concat_axis=0, tiled=True)
    back = back.reshape(frames, segs, D)
    final = (gln_gain[1] * (back.astype(F32) - center) * inv + gln_bias[1]
             + jnp.swapaxes(intra_out, 0, 1).astype(F32)).astype(BF16)
    return jnp.swapaxes(final, 0, 1)


def solution(mesh):
    in_specs = (P(("mix", "span"), None, None), P(), P(), P(), P(), P(), P(), P(), P(), P())
    out_specs = P(("mix", "span"), None, None)
    return jax.shard_map(body, mesh=mesh, in_specs=in_specs, out_specs=out_specs, check_vma=False)
```

```python
import functools
import math

import jax
import numpy as np
import jax.numpy as jnp
from jax import lax
from jax.experimental import pallas as pl
from jax.experimental.pallas import tpu as pltpu
from jax.sharding import PartitionSpec as P

D = 256
HEADS = 8
HD = D // HEADS
FF = 1024
EPS = 1e-05
AUG = HD + 16
F32 = jnp.float32
BF16 = jnp.bfloat16


def pos_parts(length):
    column = np.arange(D)
    rates = np.exp(-(2 * (column // 2)) / D * math.log(10000.0))[:, None]
    near = np.arange(128)[None, :] * rates
    far = 128 * np.arange(length // 128)[None, :] * rates
    even = (column % 2 == 0)[:, None]
    outer = np.where(even, np.sin(far), np.cos(far))
    swap = np.where(even, np.cos(far), -np.sin(far))
    far_two = np.zeros((2 * D, 128))
    far_two[:, : length // 128] = np.concatenate([outer, swap], axis=0)
    return np.stack([np.cos(near), np.sin(near)]).astype(np.float32), far_two.astype(np.float32)


def dot(a, b):
    return lax.dot_general(a, b, (((1,), (0,)), ((), ())), preferred_element_type=F32)


def norm_cols(x, gain):
    center = jnp.mean(x, axis=0, keepdims=True)
    shifted = x - center
    spread = jnp.mean(shifted * shifted, axis=0, keepdims=True)
    return shifted * lax.rsqrt(spread + EPS) * gain


CHUNK = 256
LEAD = 2
TRAIL = 1


def score_unit(q_t, keys, c, h):
    block, at = divmod(h * HD, 128)
    parts = []
    if at:
        parts.append(jnp.zeros((at, CHUNK), BF16))
    parts.append(q_t[h * HD : (h + 1) * HD, c * CHUNK : (c + 1) * CHUNK])
    if at + HD < 128:
        parts.append(jnp.zeros((128 - at - HD, CHUNK), BF16))
    return dot(keys[:, block * 128 : (block + 1) * 128], jnp.concatenate(parts, axis=0))


def run_step(fills, b, scores, weights, ctx):
    if b is None:
        for piece in fills:
            piece()
        return
    x_res, q_t, keys, vaug, after, wo_t = b
    units = [(c, h) for c in range(q_t.shape[1] // CHUNK) for h in range(HEADS)]
    tops = {}
    n = len(units)
    slots = n + LEAD + TRAIL
    done = 0
    for u in range(slots):
        if u < n:
            s = score_unit(q_t, keys, *units[u])
            tops[u] = jnp.max(s, axis=0, keepdims=True)
            scores[u % len(scores)][...] = s
        v = u - LEAD
        if 0 <= v < n:
            s = scores[v % len(scores)][...]
            weights[v % len(weights)][...] = jnp.exp2(s - tops.pop(v)).astype(BF16)
        w = v - TRAIL
        if 0 <= w < n:
            c, h = units[w]
            mixed = dot(vaug[h * AUG : (h + 1) * AUG, :], weights[w % len(weights)][...])
            ctx[h * HD : (h + 1) * HD, c * CHUNK : (c + 1) * CHUNK] = (
                mixed[:HD, :] * (1.0 / mixed[HD : HD + 1, :])
            ).astype(BF16)
        upto = len(fills) * (u + 1) // slots
        for piece in fills[done:upto]:
            piece()
        done = upto
    after[...] = x_res[...] + dot(wo_t[...], ctx[...])


def pieces_a(x, pos, g1, wq_t, wv_t, w_k, x_res, q_t, keys, vaug, n1):
    def first():
        xt = x().T.astype(F32) + pos[...]
        x_res[...] = xt
        n1[...] = norm_cols(xt, g1).astype(BF16)

    def get_keys():
        keys[...] = dot(n1[...].T, w_k[...]).astype(BF16)

    def get_queries():
        scale = math.log2(math.e) / math.sqrt(HD)
        q_t[...] = (dot(wq_t[...], n1[...]) * scale).astype(BF16)

    def get_values():
        v_t = dot(wv_t[...], n1[...]).astype(BF16)
        for h in range(HEADS):
            vaug[h * AUG : h * AUG + HD, :] = v_t[h * HD : (h + 1) * HD, :]

    return [first, get_keys, get_queries, get_values]


def pieces_c(after, g2, wup_t, wdn_t, y_ref, sums, n2, hidden):
    def first():
        n2[...] = norm_cols(after[...], g2).astype(BF16)

    def up(j):
        rows = slice(j * D, (j + 1) * D)
        hidden[rows, :] = jnp.maximum(dot(wup_t[rows, :], n2[...]), 0.0).astype(BF16)

    def down():
        y_t = after[...] + dot(wdn_t[...], hidden[...])
        part = y_t.reshape(D // 8, 8, y_t.shape[1])
        for k in range(y_t.shape[1] // 128):
            lanes = slice(k * 128, (k + 1) * 128)
            sums[0] += jnp.sum(part[:, :, lanes], axis=0)
            sums[1] += jnp.sum(part[:, :, lanes] * part[:, :, lanes], axis=0)
        y_ref[...] = y_t.astype(BF16).T.reshape(y_ref.shape)

    return [first] + [functools.partial(up, j) for j in range(FF // D)] + [down]


def layer_kernel(pair, x_ref, near_ref, far_ref, gain_ref, wq_ref, wk_ref, wv_ref, wo_ref, wup_ref, wdn_ref,
                 y_ref, stat_ref, wq_t, wv_t, wo_t, wup_t, wdn_t, pos, g1, g2, n1, n2, hidden, sums, *bufs):
    length = pos.shape[1]
    slots = (bufs[0:5], bufs[5:10])
    ctx, scores, weights = bufs[10], bufs[11 : 12 + LEAD], bufs[12 + LEAD :]
    step, last = pl.program_id(0), pl.num_programs(0) - 1

    def run(sub, a, b, c):
        here, other = slots[sub], slots[1 - sub]
        left, right = [], []
        if c:
            left = pieces_c(here[4], g2[:, :1], wup_t, wdn_t, pair(y_ref, sub), sums, n2, hidden)
        if a:
            get = lambda: pair(x_ref, sub)[...].reshape(length, D)
            right = pieces_a(get, pos, g1[:, :1], wq_t, wv_t, wk_ref, *here[:4], n1)
        fills = []
        while left or right:
            fills += left[:1] + right[:1]
            left, right = left[1:], right[1:]
        run_step(fills, (*other, wo_t) if b else None, scores, weights, ctx)

    @pl.when(step == 0)
    def _():
        wq_t[...] = wq_ref[...].T
        wv_t[...] = wv_ref[...].T
        wo_t[...] = wo_ref[...].T
        wup_t[...] = wup_ref[...].T
        wdn_t[...] = wdn_ref[...].T
        g1[...] = jnp.broadcast_to(gain_ref[0:1, :], (128, D)).T
        g2[...] = jnp.broadcast_to(gain_ref[1:2, :], (128, D)).T
        for a in range(length // 128):
            pos[:, a * 128 : (a + 1) * 128] = (
                far_ref[:D, a : a + 1] * near_ref[0] + far_ref[D:, a : a + 1] * near_ref[1])
        for slot in slots:
            slot[3][...] = jnp.ones_like(slot[3])
        sums[...] = jnp.zeros_like(sums)
        run(0, True, False, False)
        run(1, True, True, False)

    @pl.when((step > 0) & (step < last))
    def _():
        run(0, True, True, True)
        run(1, True, True, True)

    @pl.when(step == last)
    def _():
        run(0, False, True, True)
        run(1, False, False, True)
        rows = [jnp.sum(sums[k], axis=0, keepdims=True) for k in range(2)]
        tile = jnp.concatenate(rows + [jnp.zeros((6, 128), F32)], axis=0)
        stat_ref[...] = jnp.broadcast_to(tile[None], stat_ref.shape)


def layer(x, count, x_block, x_map, pair, length, level, gain, weights, peers, name):
    near, far = pos_parts(length)
    pick = lambda a: pl.BlockSpec((None, *a.shape[1:]), lambda i: (level,) + (0,) * (a.ndim - 1))
    whole = lambda a: pl.BlockSpec(a.shape, lambda i: (0,) * a.ndim)
    pairs = count // 2
    slot = [
        pltpu.VMEM((D, length), F32), pltpu.VMEM((D, length), BF16), pltpu.VMEM((length, D), BF16),
        pltpu.VMEM((HEADS * AUG, length), BF16), pltpu.VMEM((D, length), F32),
    ]
    return pl.pallas_call(
        functools.partial(layer_kernel, pair),
        grid=(pairs + 1,),
        in_specs=[pl.BlockSpec(x_block, lambda i: x_map(jnp.minimum(i, pairs - 1))),
                  whole(near), whole(far), pick(gain)] + [pick(w) for w in weights],
        out_specs=[pl.BlockSpec(x_block, lambda i: x_map(jnp.maximum(i - 1, 0))),
                   pl.BlockSpec((peers, 8, 128), lambda i: (0, 0, 0))],
        out_shape=[jax.ShapeDtypeStruct(x.shape, BF16), jax.ShapeDtypeStruct((peers, 8, 128), F32)],
        scratch_shapes=[
            pltpu.VMEM((D, D), BF16), pltpu.VMEM((D, D), BF16), pltpu.VMEM((D, D), BF16),
            pltpu.VMEM((FF, D), BF16), pltpu.VMEM((D, FF), BF16),
            pltpu.VMEM((D, length), F32), pltpu.VMEM((D, 128), F32), pltpu.VMEM((D, 128), F32),
            pltpu.VMEM((D, length), BF16), pltpu.VMEM((D, length), BF16), pltpu.VMEM((FF, length), BF16),
            pltpu.VMEM((2, 8, 128), F32), *slot, *slot, pltpu.VMEM((D, length), BF16),
            *[pltpu.VMEM((length, CHUNK), F32)] * (LEAD + 1), *[pltpu.VMEM((length, CHUNK), BF16)] * (TRAIL + 1),
        ],
        compiler_params=pltpu.CompilerParams(dimension_semantics=("arbitrary",)),
        name=name,
    )(x, jnp.asarray(near), jnp.asarray(far), gain, *weights)


def blend_kernel(cells, stat_ref, out_ref, res_ref, gain_ref, bias_ref, final_ref):
    parts = jnp.sum(stat_ref[...], axis=0)
    center = jnp.sum(parts[0:1, :], axis=1, keepdims=True) / cells
    spread = jnp.sum(parts[1:2, :], axis=1, keepdims=True) / cells - center * center
    slope = gain_ref[...] * lax.rsqrt(spread + EPS)
    shifted = out_ref[...].astype(F32) - center[None]
    final = slope[None] * shifted + bias_ref[...][None] + res_ref[...].astype(F32)
    final_ref[...] = jnp.swapaxes(final, 0, 1).astype(BF16)


def blend(stat, out, residual, gain, bias, cells, in_block, in_map, steps, name):
    first, second, _ = out.shape
    block = pl.BlockSpec(in_block, in_map)
    whole = lambda a: pl.BlockSpec(a.shape, lambda i: (0,) * a.ndim)
    def out_map(i):
        one, two, _ = in_map(i)
        return two, one, 0
    return pl.pallas_call(
        functools.partial(blend_kernel, cells),
        grid=(steps,),
        in_specs=[whole(stat), block, block, whole(gain), whole(bias)],
        out_specs=pl.BlockSpec((in_block[1], in_block[0], D), out_map),
        out_shape=jax.ShapeDtypeStruct((second, first, D), BF16),
        compiler_params=pltpu.CompilerParams(dimension_semantics=("arbitrary",)),
        name=name,
    )(stat, out, residual, gain, bias)


def body(mixture, w_query, w_key, w_value, w_out, w_up, w_down, ln_gain, gln_gain, gln_bias):
    shards = lax.axis_size("span")
    segs, frames, _ = mixture.shape
    own = frames // shards
    total = segs * shards
    cells = float(total * frames * D)
    weights = (w_query, w_key, w_value, w_out, w_up, w_down)
    steps = 4

    intra, stat = layer(mixture, segs, (2, frames, D), lambda i: (i, 0, 0), lambda r, k: r.at[k], frames,
                        0, ln_gain, weights, shards, name="intra")
    stat = lax.all_to_all(stat, "span", split_axis=0, concat_axis=0, tiled=True)
    across = blend(stat, intra, mixture, gln_gain[0:1], gln_bias[0:1], cells,
                   (segs, frames // steps, D), lambda i: (0, i, 0), steps, "blend_intra")
    moved = lax.all_to_all(across.reshape(shards, own, segs, D), "span", split_axis=0, concat_axis=0, tiled=True)

    inter, stat = layer(moved, own, (shards, 2, segs, D), lambda i: (0, i, 0, 0), lambda r, k: r.at[:, k], total,
                        1, ln_gain, weights, 1, name="inter")
    back = lax.all_to_all(inter, "span", split_axis=0, concat_axis=0, tiled=True)
    stat = stat[0]
    for bit in range(shards.bit_length() - 1):
        stat = stat + lax.ppermute(stat, "span", [(i, i ^ (1 << bit)) for i in range(shards)])
    return blend(stat[None], back.reshape(frames, segs, D), across, gln_gain[1:2], gln_bias[1:2], cells,
                 (frames // steps, segs, D), lambda i: (i, 0, 0), steps, "blend_inter")


def solution(mesh):
    in_specs = (P(("mix", "span"), None, None), P(), P(), P(), P(), P(), P(), P(), P(), P())
    out_specs = P(("mix", "span"), None, None)
    return jax.shard_map(body, mesh=mesh, in_specs=in_specs, out_specs=out_specs, check_vma=False)
```

```python
import functools
import math

import jax
import numpy as np
import jax.numpy as jnp
from jax import lax
from jax.experimental import pallas as pl
from jax.experimental.pallas import tpu as pltpu
from jax.sharding import PartitionSpec as P

D = 256
HEADS = 8
HD = D // HEADS
FF = 1024
EPS = 1e-05
AUG = HD + 16
F32 = jnp.float32
BF16 = jnp.bfloat16


def pos_parts(length):
    column = np.arange(D)
    rates = np.exp(-(2 * (column // 2)) / D * math.log(10000.0))[:, None]
    near = np.arange(128)[None, :] * rates
    far = 128 * np.arange(length // 128)[None, :] * rates
    even = (column % 2 == 0)[:, None]
    outer = np.where(even, np.sin(far), np.cos(far))
    swap = np.where(even, np.cos(far), -np.sin(far))
    far_two = np.zeros((2 * D, 128))
    far_two[:, : length // 128] = np.concatenate([outer, swap], axis=0)
    return np.stack([np.cos(near), np.sin(near)]).astype(np.float32), far_two.astype(np.float32)


def dot(a, b):
    return lax.dot_general(a, b, (((1,), (0,)), ((), ())), preferred_element_type=F32)


def norm_cols(x, gain):
    center = jnp.mean(x, axis=0, keepdims=True)
    shifted = x - center
    spread = jnp.mean(shifted * shifted, axis=0, keepdims=True)
    return shifted * lax.rsqrt(spread + EPS) * gain


CHUNK = 256
LEAD = 2
TRAIL = 1


def score_unit(q_t, keys, c, h):
    block, at = divmod(h * HD, 128)
    parts = []
    if at:
        parts.append(jnp.zeros((at, CHUNK), BF16))
    parts.append(q_t[h * HD : (h + 1) * HD, c * CHUNK : (c + 1) * CHUNK])
    if at + HD < 128:
        parts.append(jnp.zeros((128 - at - HD, CHUNK), BF16))
    return dot(keys[:, block * 128 : (block + 1) * 128], jnp.concatenate(parts, axis=0))


def run_step(fills, b, scores, weights, ctx):
    if b is None:
        for piece in fills:
            piece()
        return
    x_res, q_t, keys, vaug, after, wo_t = b
    units = [(c, h) for c in range(q_t.shape[1] // CHUNK) for h in range(HEADS)]
    tops = {}
    n = len(units)
    slots = n + LEAD + TRAIL
    done = 0
    for u in range(slots):
        if u < n:
            s = score_unit(q_t, keys, *units[u])
            tops[u] = jnp.max(s, axis=0, keepdims=True)
            scores[u % len(scores)][...] = s
        v = u - LEAD
        if 0 <= v < n:
            s = scores[v % len(scores)][...]
            weights[v % len(weights)][...] = jnp.exp2(s - tops.pop(v)).astype(BF16)
        w = v - TRAIL
        if 0 <= w < n:
            c, h = units[w]
            mixed = dot(vaug[h * AUG : (h + 1) * AUG, :], weights[w % len(weights)][...])
            ctx[h * HD : (h + 1) * HD, c * CHUNK : (c + 1) * CHUNK] = (
                mixed[:HD, :] * (1.0 / mixed[HD : HD + 1, :])
            ).astype(BF16)
        upto = len(fills) * (u + 1) // slots
        for piece in fills[done:upto]:
            piece()
        done = upto
    after[...] = x_res[...] + dot(wo_t[...], ctx[...])


def pieces_a(x, pos, g1, wq_t, wv_t, w_k, x_res, q_t, keys, vaug, n1):
    def first():
        xt = x().T.astype(F32) + pos[...]
        x_res[...] = xt
        n1[...] = norm_cols(xt, g1).astype(BF16)

    def get_keys():
        keys[...] = dot(n1[...].T, w_k[...]).astype(BF16)

    def get_queries():
        scale = math.log2(math.e) / math.sqrt(HD)
        q_t[...] = (dot(wq_t[...], n1[...]) * scale).astype(BF16)

    def get_values():
        v_t = dot(wv_t[...], n1[...]).astype(BF16)
        for h in range(HEADS):
            vaug[h * AUG : h * AUG + HD, :] = v_t[h * HD : (h + 1) * HD, :]

    return [first, get_keys, get_queries, get_values]


def pieces_c(after, g2, wup_t, wdn_t, y_ref, sums, n2, hidden):
    def first():
        n2[...] = norm_cols(after[...], g2).astype(BF16)

    def up(j):
        rows = slice(j * D, (j + 1) * D)
        hidden[rows, :] = jnp.maximum(dot(wup_t[rows, :], n2[...]), 0.0).astype(BF16)

    def down():
        y_t = after[...] + dot(wdn_t[...], hidden[...])
        part = y_t.reshape(D // 8, 8, y_t.shape[1])
        for k in range(y_t.shape[1] // 128):
            lanes = slice(k * 128, (k + 1) * 128)
            sums[0] += jnp.sum(part[:, :, lanes], axis=0)
            sums[1] += jnp.sum(part[:, :, lanes] * part[:, :, lanes], axis=0)
        y_ref[...] = y_t.astype(BF16).T.reshape(y_ref.shape)

    return [first] + [functools.partial(up, j) for j in range(FF // D)] + [down]


def layer_kernel(pair, pairs, joined, x_ref, near_ref, far_ref, gain_ref, wq_ref, wk_ref, wv_ref, wo_ref, wup_ref, wdn_ref,
                 y_ref, *refs):
    if joined:
        stat_ref = None
    else:
        stat_ref, refs = refs[0], refs[1:]
    layer_steps(pair, pairs, x_ref, near_ref, far_ref, gain_ref, wq_ref, wk_ref, wv_ref, wo_ref, wup_ref, wdn_ref,
                y_ref, stat_ref, *refs)


def layer_steps(pair, pairs, x_ref, near_ref, far_ref, gain_ref, wq_ref, wk_ref, wv_ref, wo_ref, wup_ref, wdn_ref,
                y_ref, stat_ref, wq_t, wv_t, wo_t, wup_t, wdn_t, pos, g1, g2, n1, n2, hidden, sums, *bufs):
    length = pos.shape[1]
    slots = (bufs[0:5], bufs[5:10])
    ctx, scores, weights = bufs[10], bufs[11 : 12 + LEAD], bufs[12 + LEAD :]
    step, last = pl.program_id(0), pairs

    def out_part(sub):
        if stat_ref is not None:
            return pair(y_ref, sub)
        half = y_ref.shape[1] // 2
        return y_ref.at[:, sub * half : (sub + 1) * half]

    def run(sub, a, b, c):
        here, other = slots[sub], slots[1 - sub]
        left, right = [], []
        if c:
            left = pieces_c(here[4], g2[:, :1], wup_t, wdn_t, out_part(sub), sums, n2, hidden)
        if a:
            get = lambda: pair(x_ref, sub)[...].reshape(length, D)
            right = pieces_a(get, pos, g1[:, :1], wq_t, wv_t, wk_ref, *here[:4], n1)
        fills = []
        while left or right:
            fills += left[:1] + right[:1]
            left, right = left[1:], right[1:]
        run_step(fills, (*other, wo_t) if b else None, scores, weights, ctx)

    @pl.when(step == 0)
    def _():
        wq_t[...] = wq_ref[...].T
        wv_t[...] = wv_ref[...].T
        wo_t[...] = wo_ref[...].T
        wup_t[...] = wup_ref[...].T
        wdn_t[...] = wdn_ref[...].T
        g1[...] = jnp.broadcast_to(gain_ref[0:1, :], (128, D)).T
        g2[...] = jnp.broadcast_to(gain_ref[1:2, :], (128, D)).T
        for a in range(length // 128):
            pos[:, a * 128 : (a + 1) * 128] = (
                far_ref[:D, a : a + 1] * near_ref[0] + far_ref[D:, a : a + 1] * near_ref[1])
        for slot in slots:
            slot[3][...] = jnp.ones_like(slot[3])
        sums[...] = jnp.zeros_like(sums)
        run(0, True, False, False)
        run(1, True, True, False)

    @pl.when((step > 0) & (step < last))
    def _():
        run(0, True, True, True)
        run(1, True, True, True)

    @pl.when(step == last)
    def _():
        run(0, False, True, True)
        run(1, False, False, True)
        if stat_ref is not None:
            rows = [jnp.sum(sums[k], axis=0, keepdims=True) for k in range(2)]
            tile = jnp.concatenate(rows + [jnp.zeros((6, 128), F32)], axis=0)
            stat_ref[...] = jnp.broadcast_to(tile[None], stat_ref.shape)

    if stat_ref is None:
        @pl.when(step == last + 1)
        def _():
            rows = [jnp.sum(sums[k], axis=0, keepdims=True) for k in range(2)]
            terms = [t.astype(F32) for r in rows for t in split_three(r)]
            tile = jnp.concatenate(terms + [jnp.zeros((y_ref.shape[1] - 6, 128), F32)], axis=0)
            tile = jnp.concatenate([tile, jnp.zeros_like(tile)], axis=1).astype(BF16)
            y_ref[...] = jnp.broadcast_to(tile[None], y_ref.shape)


def layer(x, count, x_block, x_map, pair, length, level, gain, weights, joined, peers, name):
    near, far = pos_parts(length)
    pick = lambda a: pl.BlockSpec((None, *a.shape[1:]), lambda i: (level,) + (0,) * (a.ndim - 1))
    whole = lambda a: pl.BlockSpec(a.shape, lambda i: (0,) * a.ndim)
    pairs = count // 2
    slot = [
        pltpu.VMEM((D, length), F32), pltpu.VMEM((D, length), BF16), pltpu.VMEM((length, D), BF16),
        pltpu.VMEM((HEADS * AUG, length), BF16), pltpu.VMEM((D, length), F32),
    ]
    if joined is None:
        steps = pairs + 1
        out_specs = [pl.BlockSpec(x_block, lambda i: x_map(jnp.maximum(i - 1, 0))),
                     pl.BlockSpec((peers, 8, 128), lambda i: (0, 0, 0))]
        out_shape = [jax.ShapeDtypeStruct(x.shape, BF16), jax.ShapeDtypeStruct((peers, 8, 128), F32)]
    else:
        steps = pairs + 2
        out_specs = pl.BlockSpec((peers, (joined[1] - 8) // pairs, D), lambda i: (0, jnp.maximum(i - 1, 0), 0))
        out_shape = jax.ShapeDtypeStruct(joined, BF16)
    return pl.pallas_call(
        functools.partial(layer_kernel, pair, pairs, joined is not None),
        grid=(steps,),
        in_specs=[pl.BlockSpec(x_block, lambda i: x_map(jnp.minimum(i, pairs - 1))),
                  whole(near), whole(far), pick(gain)] + [pick(w) for w in weights],
        out_specs=out_specs,
        out_shape=out_shape,
        scratch_shapes=[
            pltpu.VMEM((D, D), BF16), pltpu.VMEM((D, D), BF16), pltpu.VMEM((D, D), BF16),
            pltpu.VMEM((FF, D), BF16), pltpu.VMEM((D, FF), BF16),
            pltpu.VMEM((D, length), F32), pltpu.VMEM((D, 128), F32), pltpu.VMEM((D, 128), F32),
            pltpu.VMEM((D, length), BF16), pltpu.VMEM((D, length), BF16), pltpu.VMEM((FF, length), BF16),
            pltpu.VMEM((2, 8, 128), F32), *slot, *slot, pltpu.VMEM((D, length), BF16),
            *[pltpu.VMEM((length, CHUNK), F32)] * (LEAD + 1), *[pltpu.VMEM((length, CHUNK), BF16)] * (TRAIL + 1),
        ],
        compiler_params=pltpu.CompilerParams(dimension_semantics=("arbitrary",)),
        name=name,
    )(x, jnp.asarray(near), jnp.asarray(far), gain, *weights)


def split_three(x):
    high = x.astype(BF16)
    rest = x - high.astype(F32)
    mid = rest.astype(BF16)
    return high, mid, (rest - mid.astype(F32)).astype(BF16)


class ByFrame:
    def __init__(self, ref, own, segs):
        self.ref, self.own, self.segs = ref, own, segs

    def __getitem__(self, i):
        peer, frame = divmod(i, self.own)
        return self.ref[peer, frame * self.segs : (frame + 1) * self.segs, :]


def blend_kernel(cells, level, stat_ref, out_ref, res_ref, gain_ref, bias_ref, final_ref, *halves):
    if stat_ref.dtype == BF16:
        rows = jnp.sum(stat_ref[...].astype(F32), axis=0)
        sums = [jnp.sum(rows[3 * k : 3 * k + 3, :], axis=(0, 1), keepdims=True) for k in range(2)]
    else:
        rows = jnp.sum(stat_ref[...], axis=0)
        sums = [jnp.sum(rows[k : k + 1, :], axis=(0, 1), keepdims=True) for k in range(2)]
    center = sums[0] / cells
    spread = sums[1] / cells - center * center
    slope = gain_ref[level : level + 1, :] * lax.rsqrt(spread + EPS)
    one, two, _ = res_ref.shape
    pitch = two + 8
    for i in range(one):
        data = out_ref[i].astype(F32) - center
        final = slope * data + bias_ref[level : level + 1, :] + res_ref[i].astype(F32)
        for k, half in enumerate(halves):
            half[i * pitch : i * pitch + two, :] = final[:, k * 128 : (k + 1) * 128]
    for j in range(two):
        for k, half in enumerate(halves):
            final_ref[j, :, k * 128 : (k + 1) * 128] = half[pl.ds(j, one, stride=pitch), :].astype(BF16)


def blend(stat, stat_spec, out, out_spec, out_view, residual, res_block, res_map, gain, bias, level, cells, steps, name):
    first, second, _ = residual.shape
    whole = lambda a: pl.BlockSpec(a.shape, lambda i: (0,) * a.ndim)

    def final_map(i):
        one, two, _ = res_map(i)
        return two, one, 0

    def kernel(stat_ref, out_ref, *rest):
        blend_kernel(cells, level, stat_ref, out_view(out_ref), *rest)

    return pl.pallas_call(
        kernel,
        grid=(steps,),
        in_specs=[stat_spec, out_spec, pl.BlockSpec(res_block, res_map), whole(gain), whole(bias)],
        out_specs=pl.BlockSpec((res_block[1], res_block[0], D), final_map),
        out_shape=jax.ShapeDtypeStruct((second, first, D), BF16),
        scratch_shapes=[pltpu.VMEM((res_block[0] * (res_block[1] + 8), 128), F32)] * 2,
        compiler_params=pltpu.CompilerParams(dimension_semantics=("arbitrary",)),
        name=name,
    )(stat, out, residual, gain, bias)


def body(mixture, w_query, w_key, w_value, w_out, w_up, w_down, ln_gain, gln_gain, gln_bias):
    shards = lax.axis_size("span")
    segs, frames, _ = mixture.shape
    own = frames // shards
    total = segs * shards
    cells = float(total * frames * D)
    weights = (w_query, w_key, w_value, w_out, w_up, w_down)
    steps = 4

    intra, stat = layer(mixture, segs, (2, frames, D), lambda i: (i, 0, 0), lambda r, k: r.at[k], frames,
                        0, ln_gain, weights, None, shards, name="intra")
    stat = lax.all_to_all(stat, "span", split_axis=0, concat_axis=0, tiled=True)
    block = (segs, frames // steps, D)
    spread = lambda i: (0, i, 0)
    across = blend(stat, pl.BlockSpec(stat.shape, lambda i: (0, 0, 0)), intra, pl.BlockSpec(block, spread), lambda r: r,
                   mixture, block, spread, gln_gain, gln_bias, 0, cells, steps, "blend_intra")
    moved = lax.all_to_all(across.reshape(shards, own, segs, D), "span", split_axis=0, concat_axis=0, tiled=True)

    rows = own * segs
    inter = layer(moved, own, (shards, 2, segs, D), lambda i: (0, i, 0, 0), lambda r, k: r.at[:, k], total,
                  1, ln_gain, weights, (shards, rows + 8, D), shards, name="inter")
    back = lax.all_to_all(inter, "span", split_axis=0, concat_axis=0, tiled=True)
    peers = shards // steps
    return blend(back, pl.BlockSpec((shards, 8, D), lambda i: (0, rows // 8, 0)),
                 back, pl.BlockSpec((peers, rows, D), lambda i: (i, 0, 0)), lambda r: ByFrame(r, own, segs),
                 across, (frames // steps, segs, D), lambda i: (i, 0, 0), gln_gain, gln_bias, 1, cells, steps, "blend_inter")


def solution(mesh):
    in_specs = (P(("mix", "span"), None, None), P(), P(), P(), P(), P(), P(), P(), P(), P())
    out_specs = P(("mix", "span"), None, None)
    return jax.shard_map(body, mesh=mesh, in_specs=in_specs, out_specs=out_specs, check_vma=False)
```

```python
import functools
import math

import jax
import numpy as np
import jax.numpy as jnp
from jax import lax
from jax.experimental import pallas as pl
from jax.experimental.pallas import tpu as pltpu
from jax.sharding import PartitionSpec as P


D = 256
HEADS = 8
HD = D // HEADS
FF = 1024
EPS = 1e-05
AUG = HD + 16
F32 = jnp.float32
BF16 = jnp.bfloat16


def pos_parts():
    column = np.arange(D)
    rates = np.exp(-(2 * (column // 2)) / D * math.log(10000.0))[:, None]
    near = np.arange(128)[None, :] * rates
    far = 128 * np.arange(8)[None, :] * rates
    even = (column % 2 == 0)[:, None]
    outer = np.where(even, np.sin(far), np.cos(far))
    swap = np.where(even, np.cos(far), -np.sin(far))
    return (np.stack([np.cos(near), np.sin(near)]).astype(np.float32),
            np.concatenate([outer, swap], axis=0).T.astype(np.float32))


def dot(a, b):
    return lax.dot_general(a, b, (((1,), (0,)), ((), ())), preferred_element_type=F32)


def norm_cols(x, gain):
    center = jnp.mean(x, axis=0, keepdims=True)
    shifted = x - center
    spread = jnp.mean(shifted * shifted, axis=0, keepdims=True)
    return shifted * lax.rsqrt(spread + EPS) * gain


CHUNK = 256
LEAD = 2
TRAIL = 1


def score_unit(q_t, keys, c, h):
    block, at = divmod(h * HD, 128)
    parts = []
    if at:
        parts.append(jnp.zeros((at, CHUNK), BF16))
    parts.append(q_t[h * HD : (h + 1) * HD, c * CHUNK : (c + 1) * CHUNK])
    if at + HD < 128:
        parts.append(jnp.zeros((128 - at - HD, CHUNK), BF16))
    return dot(keys[:, block * 128 : (block + 1) * 128], jnp.concatenate(parts, axis=0))


def run_step(fills, b, scores, weights, ctx):
    if b is None:
        for piece in fills:
            piece()
        return
    x_res, q_t, keys, vaug, after, wo_t = b
    units = [(c, h) for c in range(q_t.shape[1] // CHUNK) for h in range(HEADS)]
    tops = {}
    n = len(units)
    slots = n + LEAD + TRAIL
    done = 0
    for u in range(slots):
        if u < n:
            s = score_unit(q_t, keys, *units[u])
            tops[u] = jnp.max(s, axis=0, keepdims=True)
            scores[u % len(scores)][...] = s
        v = u - LEAD
        if 0 <= v < n:
            s = scores[v % len(scores)][...]
            weights[v % len(weights)][...] = jnp.exp2(s - tops.pop(v)).astype(BF16)
        w = v - TRAIL
        if 0 <= w < n:
            c, h = units[w]
            mixed = dot(vaug[h * AUG : (h + 1) * AUG, :], weights[w % len(weights)][...])
            ctx[h * HD : (h + 1) * HD, c * CHUNK : (c + 1) * CHUNK] = (
                mixed[:HD, :] * (1.0 / mixed[HD : HD + 1, :])
            ).astype(BF16)
        upto = len(fills) * (u + 1) // slots
        for piece in fills[done:upto]:
            piece()
        done = upto
    after[...] = x_res[...] + dot(wo_t[...], ctx[...])


def pieces_a(x, pos, g1, wq_t, wv_t, w_k, x_res, q_t, keys, vaug, n1):
    def first():
        xt = x().T.astype(F32) + pos[...]
        x_res[...] = xt
        n1[...] = norm_cols(xt, g1).astype(BF16)

    def get_keys():
        keys[...] = dot(n1[...].T, w_k[...]).astype(BF16)

    def get_queries():
        scale = math.log2(math.e) / math.sqrt(HD)
        q_t[...] = (dot(wq_t[...], n1[...]) * scale).astype(BF16)

    def get_values():
        v_t = dot(wv_t[...], n1[...]).astype(BF16)
        for h in range(HEADS):
            vaug[h * AUG : h * AUG + HD, :] = v_t[h * HD : (h + 1) * HD, :]

    return [first, get_keys, get_queries, get_values]


def global_norm(rows, gain, bias, cells):
    total = [jnp.sum(rows[3 * k : 3 * k + 3, :], axis=(0, 1), keepdims=True) for k in range(2)]
    center = total[0] / cells
    spread = total[1] / cells - center * center
    slope = gain * lax.rsqrt(spread + EPS)
    return slope, bias - slope * center


def split_three(x):
    high = x.astype(BF16)
    rest = x - high.astype(F32)
    mid = rest.astype(BF16)
    return high, mid, (rest - mid.astype(F32)).astype(BF16)


def stat_rows(sums, count):
    terms = [t.astype(F32) for k in range(2) for t in split_three(jnp.sum(sums[k], axis=0, keepdims=True))]
    tile = jnp.concatenate(terms + [jnp.zeros((count - 6, 128), F32)], axis=0)
    return jnp.concatenate([tile, jnp.zeros_like(tile)], axis=1).astype(BF16)


def pieces_c(after, g2, wup_t, wdn_t, emit, sums, valid, n2, hidden):
    def first():
        n2[...] = norm_cols(after[...], g2).astype(BF16)

    def up(j):
        rows = slice(j * D, (j + 1) * D)
        hidden[rows, :] = jnp.maximum(dot(wup_t[rows, :], n2[...]), 0.0).astype(BF16)

    def down():
        y_t = after[...] + dot(wdn_t[...], hidden[...])
        part = y_t.reshape(D // 8, 8, y_t.shape[1])
        for k in range(y_t.shape[1] // 128):
            lanes = slice(k * 128, (k + 1) * 128)
            sums[0] += jnp.where(valid, jnp.sum(part[:, :, lanes], axis=0), 0.0)
            sums[1] += jnp.where(valid, jnp.sum(part[:, :, lanes] * part[:, :, lanes], axis=0), 0.0)
        emit(y_t.astype(BF16).T)

    return [first] + [functools.partial(up, j) for j in range(FF // D)] + [down]


def layer_steps(pairs, prepare, get, emit, near_ref, far_ref, gain_ref, wq_ref, wk_ref, wv_ref, wo_ref, wup_ref, wdn_ref,
                wq_t, wv_t, wo_t, wup_t, wdn_t, pos, g1, g2, n1, n2, hidden, sums, *bufs):
    length = pos.shape[1]
    slots = (bufs[0:5], bufs[5:10])
    ctx, scores, weights = bufs[10], bufs[11 : 12 + LEAD], bufs[12 + LEAD :]
    step = pl.program_id(0)

    def run(sub, a, b, c):
        here, other = slots[sub], slots[1 - sub]
        left, right = [], []
        if c:
            left = pieces_c(here[4], g2[:, :1], wup_t, wdn_t, functools.partial(emit, sub), sums, step > 0, n2, hidden)
        if a:
            right = pieces_a(lambda: get(sub), pos, g1[:, :1], wq_t, wv_t, wk_ref, *here[:4], n1)
        fills = []
        while left or right:
            fills += left[:1] + right[:1]
            left, right = left[1:], right[1:]
        run_step(fills, (*other, wo_t) if b else None, scores, weights, ctx)

    @pl.when(step == 0)
    def _():
        wq_t[...] = wq_ref[...].T
        wv_t[...] = wv_ref[...].T
        wo_t[...] = wo_ref[...].T
        wup_t[...] = wup_ref[...].T
        wdn_t[...] = wdn_ref[...].T
        g1[...] = jnp.broadcast_to(gain_ref[0:1, :], (128, D)).T
        g2[...] = jnp.broadcast_to(gain_ref[1:2, :], (128, D)).T
        far = far_ref[...].T
        for a in range(length // 128):
            pos[:, a * 128 : (a + 1) * 128] = far[:D, a : a + 1] * near_ref[0] + far[D:, a : a + 1] * near_ref[1]
        for slot in slots:
            slot[3][...] = jnp.ones_like(slot[3])
        sums[...] = jnp.zeros_like(sums)
        prepare()
        run(0, True, False, False)

    @pl.when((step > 0) & (step <= pairs))
    def _():
        run(0, True, True, True)

    @pl.when(step < pairs)
    def _():
        run(1, True, True, True)

    @pl.when(step == pairs)
    def _():
        run(1, False, False, True)


def layer_consts(length, level, gain, weights):
    near, far = pos_parts()
    pick = lambda a: pl.BlockSpec((None, *a.shape[1:]), lambda i: (level,) + (0,) * (a.ndim - 1))
    whole = lambda a: pl.BlockSpec(a.shape, lambda i: (0,) * a.ndim)
    slot = [
        pltpu.VMEM((D, length), F32), pltpu.VMEM((D, length), BF16), pltpu.VMEM((length, D), BF16),
        pltpu.VMEM((HEADS * AUG, length), BF16), pltpu.VMEM((D, length), F32),
    ]
    scratch = [
        pltpu.VMEM((D, D), BF16), pltpu.VMEM((D, D), BF16), pltpu.VMEM((D, D), BF16),
        pltpu.VMEM((FF, D), BF16), pltpu.VMEM((D, FF), BF16),
        pltpu.VMEM((D, length), F32), pltpu.VMEM((D, 128), F32), pltpu.VMEM((D, 128), F32),
        pltpu.VMEM((D, length), BF16), pltpu.VMEM((D, length), BF16), pltpu.VMEM((FF, length), BF16),
        pltpu.VMEM((2, 8, 128), F32), *slot, *slot, pltpu.VMEM((D, length), BF16),
        *[pltpu.VMEM((length, CHUNK), F32)] * (LEAD + 1), *[pltpu.VMEM((length, CHUNK), BF16)] * (TRAIL + 1),
    ]
    values = (jnp.asarray(near), jnp.asarray(far), gain, *weights)
    specs = [whole(near), whole(far), pick(gain)] + [pick(w) for w in weights]
    return values, specs, scratch


def layer_cost(rows, length):
    dense = 2 * rows * (4 * D * D + 2 * D * FF)
    return pl.CostEstimate(flops=dense + 4 * rows * length * D, transcendentals=rows * length * HEADS,
                           bytes_accessed=4 * rows * D + 4 * D * (2 * D + FF))


PARAMS = pltpu.CompilerParams(dimension_semantics=("arbitrary",))


def intra_layer(mixture, gain, weights, peers, own):
    segs, frames, _ = mixture.shape
    half = frames // 2
    pairs, pitch = segs // 2, half + 8
    values, specs, scratch = layer_consts(frames, 0, gain, weights)

    def kernel(x_ref, *refs):
        n = len(values)
        y_ref, sent_ref = refs[n : n + 2]
        kept = refs[n + 2 : n + 4]
        work = refs[n + 4 :]
        step = pl.program_id(0)

        def emit(sub, y):
            y_ref[sub] = y
            at = pl.multiple_of(jnp.maximum(2 * step - 2 + sub, 0) * pitch, 8)
            for k, part in enumerate(kept):
                part[pl.ds(at, half), :] = y[:half, k * 128 : (k + 1) * 128].astype(F32)

        layer_steps(pairs, lambda: None, lambda sub: x_ref[sub], emit, *refs[:n], *work)

        @pl.when(step == pairs)
        def _():
            for f in range(half):
                p, j = divmod(f, own)
                for k, part in enumerate(kept):
                    sent_ref[p, j * segs : (j + 1) * segs, k * 128 : (k + 1) * 128] = (
                        part[pl.ds(f, segs, stride=pitch), :].astype(BF16))
            tile = stat_rows(work[11], 8)
            for p in range(peers):
                sent_ref[p, own * segs :, :] = tile

    rows = own * segs + 8
    return pl.pallas_call(
        kernel,
        grid=(pairs + 1,),
        in_specs=[pl.BlockSpec((2, frames, D), lambda i: (jnp.minimum(i, pairs - 1), 0, 0))] + specs,
        out_specs=[pl.BlockSpec((2, frames, D), lambda i: (jnp.maximum(i - 1, 0), 0, 0)),
                   pl.BlockSpec((peers, rows, D), lambda i: (0, 0, 0))],
        out_shape=[jax.ShapeDtypeStruct(mixture.shape, BF16), jax.ShapeDtypeStruct((peers, rows, D), BF16)],
        scratch_shapes=[pltpu.VMEM((segs * pitch, 128), F32)] * 2 + scratch,
        compiler_params=PARAMS,
        cost_estimate=layer_cost(segs * frames, frames),
        name="intra",
    )(mixture, *values)


def inter_layer(moved, sent, gln_gain, gln_bias, cells, gain, weights):
    peers, own, segs, _ = moved.shape
    total, pairs, rows = peers * segs, own // 2, own * segs
    values, specs, scratch = layer_consts(total, 1, gain, weights)
    whole = lambda a: pl.BlockSpec(a.shape, lambda i: (0,) * a.ndim)
    pick = lambda i: jnp.minimum(i, pairs - 1)
    extra, extra_specs = (), []
    if sent is not None:
        extra = (sent, sent, gln_gain, gln_bias)
        extra_specs = [pl.BlockSpec((peers, 2 * segs, D), lambda i: (0, pick(i), 0)),
                       pl.BlockSpec((peers, 8, D), lambda i: (0, rows // 8, 0)), whole(gln_gain), whole(gln_bias)]

    def kernel(x_ref, *refs):
        m, n = len(extra), len(extra) + len(values)
        y_ref, affine = refs[n : n + 2]
        work = refs[n + 2 :]
        step = pl.program_id(0)

        def prepare():
            if m:
                sums = jnp.sum(refs[1][...].astype(F32), axis=0)
                slope, offset = global_norm(sums, refs[2][0:1, :], refs[3][0:1, :], cells)
                affine[0:1, :] = slope
                affine[1:2, :] = offset

        def get(sub):
            x = x_ref[:, sub].reshape(total, D)
            if m:
                y = refs[0][:, sub * segs : (sub + 1) * segs].reshape(total, D)
                x = (affine[0:1, :] * y.astype(F32) + affine[1:2, :] + x.astype(F32)).astype(BF16)
            return x

        def emit(sub, y):
            y_ref[:, sub * segs : (sub + 1) * segs] = y.reshape(peers, segs, D)

        layer_steps(pairs, prepare, get, emit, *refs[m:n], *work)

        @pl.when(step == pairs + 1)
        def _():
            y_ref[...] = jnp.broadcast_to(stat_rows(work[11], 2 * segs)[None], y_ref.shape)

    return pl.pallas_call(
        kernel,
        grid=(pairs + 2,),
        in_specs=[pl.BlockSpec((peers, 2, segs, D), lambda i: (0, pick(i), 0, 0))] + extra_specs + specs,
        out_specs=pl.BlockSpec((peers, 2 * segs, D), lambda i: (0, jnp.maximum(i - 1, 0), 0)),
        out_shape=jax.ShapeDtypeStruct((peers, rows + 8, D), BF16),
        scratch_shapes=[pltpu.VMEM((2, D), F32)] + scratch,
        compiler_params=PARAMS,
        cost_estimate=layer_cost(rows * peers, total),
    )(moved, *extra, *values)


def blend_rest(sent, intra, mixture, gln_gain, gln_bias, cells, width):
    segs, frames, _ = mixture.shape
    half, rows = frames // 2, sent.shape[1]
    pitch = width + 8
    whole = lambda a: pl.BlockSpec(a.shape, lambda i: (0,) * a.ndim)
    block = pl.BlockSpec((segs, width, D), lambda i: (0, half // width + i, 0))

    def kernel(stat_ref, y_ref, x_ref, gain_ref, bias_ref, out_ref, *parts):
        sums = jnp.sum(stat_ref[...].astype(F32), axis=0)
        slope, offset = global_norm(sums, gain_ref[0:1, :], bias_ref[0:1, :], cells)
        for s in range(segs):
            mixed = slope * y_ref[s].astype(F32) + offset + x_ref[s].astype(F32)
            for k, part in enumerate(parts):
                part[s * pitch : s * pitch + width, :] = mixed[:, k * 128 : (k + 1) * 128]
        for f in range(width):
            for k, part in enumerate(parts):
                out_ref[f, :, k * 128 : (k + 1) * 128] = part[pl.ds(f, segs, stride=pitch), :].astype(BF16)

    return pl.pallas_call(
        kernel,
        grid=(half // width,),
        in_specs=[pl.BlockSpec((sent.shape[0], 8, D), lambda i: (0, rows // 8 - 1, 0)), block, block,
                  whole(gln_gain), whole(gln_bias)],
        out_specs=pl.BlockSpec((width, segs, D), lambda i: (i, 0, 0)),
        out_shape=jax.ShapeDtypeStruct((half, segs, D), BF16),
        scratch_shapes=[pltpu.VMEM((segs * pitch, 128), F32)] * 2,
        compiler_params=PARAMS,
        name="blend_rest",
    )(sent, intra, mixture, gln_gain, gln_bias)


def blend_final(sent, backs, intra, mixture, gln_gain, gln_bias, cells, width, own):
    segs, frames, _ = mixture.shape
    peers, rows, _ = backs[0].shape
    count, pitch = width // own, segs + 8
    steps = frames // width
    whole = lambda a: pl.BlockSpec(a.shape, lambda i: (0,) * a.ndim)
    stat_spec = pl.BlockSpec((peers, 8, D), lambda i: (0, rows // 8 - 1, 0))
    block = pl.BlockSpec((segs, width, D), lambda i: (0, i, 0))

    def kernel(stat_ref, one_ref, two_ref, first_ref, second_ref, y_ref, x_ref, gain_ref, bias_ref, out_ref, affine, *parts):
        step = pl.program_id(0)

        @pl.when(step == 0)
        def _():
            sums = jnp.sum(stat_ref[...].astype(F32), axis=0)
            affine[0:1, :], affine[1:2, :] = global_norm(sums, gain_ref[0:1, :], bias_ref[0:1, :], cells)
            sums = jnp.sum(one_ref[...].astype(F32) + two_ref[...].astype(F32), axis=0)
            affine[2:3, :], affine[3:4, :] = global_norm(sums, gain_ref[1:2, :], bias_ref[1:2, :], cells)

        def lay(ref):
            for f in range(width):
                p, j = divmod(f, own)
                z = affine[2:3, :] * ref[p, j * segs : (j + 1) * segs, :].astype(F32) + affine[3:4, :]
                for k, part in enumerate(parts):
                    part[f * pitch : f * pitch + segs, :] = z[:, k * 128 : (k + 1) * 128]

        pl.when(step < steps // 2)(lambda: lay(first_ref))
        pl.when(step >= steps // 2)(lambda: lay(second_ref))
        for s in range(segs):
            mixed = (affine[0:1, :] * y_ref[s].astype(F32) + affine[1:2, :] + x_ref[s].astype(F32)).astype(BF16)
            for k, part in enumerate(parts):
                lanes = slice(k * 128, (k + 1) * 128)
                out_ref[s, :, lanes] = (part[pl.ds(s, width, stride=pitch), :] + mixed[:, lanes].astype(F32)).astype(BF16)

    spec = lambda m: pl.BlockSpec((count, rows - 8, D), lambda i: (m(i), 0, 0))
    return pl.pallas_call(
        kernel,
        grid=(steps,),
        in_specs=[stat_spec, stat_spec, stat_spec, spec(lambda i: jnp.minimum(i, steps // 2 - 1)),
                  spec(lambda i: jnp.maximum(i - steps // 2, 0)), block, block, whole(gln_gain), whole(gln_bias)],
        out_specs=block,
        out_shape=jax.ShapeDtypeStruct(mixture.shape, BF16),
        scratch_shapes=[pltpu.VMEM((4, D), F32)] + [pltpu.VMEM((width * pitch, 128), F32)] * 2,
        compiler_params=PARAMS,
        name="blend_final",
    )(sent, backs[0], backs[1], backs[0], backs[1], intra, mixture, gln_gain, gln_bias)


def exchange(blocks):
    return lax.all_to_all(blocks, "span", split_axis=0, concat_axis=0, tiled=True)


def body(mixture, w_query, w_key, w_value, w_out, w_up, w_down, ln_gain, gln_gain, gln_bias):
    peers = lax.axis_size("span")
    segs, frames, _ = mixture.shape
    half, own = frames // 2, frames // 2 // peers
    cells = float(segs * peers * frames * D)
    weights = (w_query, w_key, w_value, w_out, w_up, w_down)

    early = exchange(jnp.swapaxes(mixture[:, :half], 0, 1).reshape(peers, own, segs, D))
    intra, sent = intra_layer(mixture, ln_gain, weights, peers, own)
    sent = exchange(sent)
    rest = blend_rest(sent, intra, mixture, gln_gain, gln_bias, cells, 32)
    rest = exchange(rest.reshape(peers, own, segs, D))
    first = inter_layer(early, sent, gln_gain, gln_bias, cells, ln_gain, weights)
    first = exchange(first)
    second = inter_layer(rest, None, None, None, cells, ln_gain, weights)
    second = exchange(second)
    return blend_final(sent, (first, second), intra, mixture, gln_gain, gln_bias, cells, 32, own)


def solution(mesh):
    in_specs = (P(("mix", "span"), None, None), P(), P(), P(), P(), P(), P(), P(), P(), P())
    out_specs = P(("mix", "span"), None, None)
    return jax.shard_map(body, mesh=mesh, in_specs=in_specs, out_specs=out_specs, check_vma=False)
```

```python
import functools
import math

import jax
import numpy as np
import jax.numpy as jnp
from jax import lax
from jax.experimental import pallas as pl
from jax.experimental.pallas import tpu as pltpu
from jax.sharding import PartitionSpec as P

D = 256
HEADS = 8
HD = D // HEADS
FF = 1024
EPS = 1e-05
AUG = HD + 16
F32 = jnp.float32
BF16 = jnp.bfloat16


def pos_parts(length):
    column = np.arange(D)
    rates = np.exp(-(2 * (column // 2)) / D * math.log(10000.0))[:, None]
    near = np.arange(128)[None, :] * rates
    far = 128 * np.arange(8)[None, :] * rates
    even = (column % 2 == 0)[:, None]
    outer = np.where(even, np.sin(far), np.cos(far))
    swap = np.where(even, np.cos(far), -np.sin(far))
    return (np.stack([np.cos(near), np.sin(near)]).astype(np.float32),
            np.concatenate([outer, swap], axis=0).T.astype(np.float32))


def dot(a, b):
    return lax.dot_general(a, b, (((1,), (0,)), ((), ())), preferred_element_type=F32)


def norm_cols(x, gain):
    center = jnp.mean(x, axis=0, keepdims=True)
    shifted = x - center
    spread = jnp.mean(shifted * shifted, axis=0, keepdims=True)
    return shifted * lax.rsqrt(spread + EPS) * gain


CHUNK = 256
LEAD = 2
TRAIL = 1


def score_unit(q_t, keys, c, h):
    block, at = divmod(h * HD, 128)
    parts = []
    if at:
        parts.append(jnp.zeros((at, CHUNK), BF16))
    parts.append(q_t[h * HD : (h + 1) * HD, c * CHUNK : (c + 1) * CHUNK])
    if at + HD < 128:
        parts.append(jnp.zeros((128 - at - HD, CHUNK), BF16))
    return dot(keys[:, block * 128 : (block + 1) * 128], jnp.concatenate(parts, axis=0))


def run_step(fills, b, scores, weights, ctx):
    if b is None:
        for piece in fills:
            piece()
        return
    x_res, q_t, keys, vaug, after, wo_t = b
    units = [(c, h) for c in range(q_t.shape[1] // CHUNK) for h in range(HEADS)]
    tops = {}
    n = len(units)
    slots = n + LEAD + TRAIL
    done = 0
    for u in range(slots):
        if u < n:
            s = score_unit(q_t, keys, *units[u])
            tops[u] = jnp.max(s, axis=0, keepdims=True)
            scores[u % len(scores)][...] = s
        v = u - LEAD
        if 0 <= v < n:
            s = scores[v % len(scores)][...]
            weights[v % len(weights)][...] = jnp.exp2(s - tops.pop(v)).astype(BF16)
        w = v - TRAIL
        if 0 <= w < n:
            c, h = units[w]
            mixed = dot(vaug[h * AUG : (h + 1) * AUG, :], weights[w % len(weights)][...])
            ctx[h * HD : (h + 1) * HD, c * CHUNK : (c + 1) * CHUNK] = (
                mixed[:HD, :] * (1.0 / mixed[HD : HD + 1, :])
            ).astype(BF16)
        upto = len(fills) * (u + 1) // slots
        for piece in fills[done:upto]:
            piece()
        done = upto
    after[...] = x_res[...] + dot(wo_t[...], ctx[...])


def pieces_a(x, pos, g1, wq_t, wv_t, w_k, x_res, q_t, keys, vaug, n1):
    def first():
        xt = x().T.astype(F32) + pos[...]
        x_res[...] = xt
        n1[...] = norm_cols(xt, g1).astype(BF16)

    def get_keys():
        keys[...] = dot(n1[...].T, w_k[...]).astype(BF16)

    def get_queries():
        scale = math.log2(math.e) / math.sqrt(HD)
        q_t[...] = (dot(wq_t[...], n1[...]) * scale).astype(BF16)

    def get_values():
        v_t = dot(wv_t[...], n1[...]).astype(BF16)
        for h in range(HEADS):
            vaug[h * AUG : h * AUG + HD, :] = v_t[h * HD : (h + 1) * HD, :]

    return [first, get_keys, get_queries, get_values]


def pieces_c(after, g2, wup_t, wdn_t, y_ref, sums, n2, hidden):
    def first():
        n2[...] = norm_cols(after[...], g2).astype(BF16)

    def up(j):
        rows = slice(j * D, (j + 1) * D)
        hidden[rows, :] = jnp.maximum(dot(wup_t[rows, :], n2[...]), 0.0).astype(BF16)

    def down():
        y_t = after[...] + dot(wdn_t[...], hidden[...])
        part = y_t.reshape(D // 8, 8, y_t.shape[1])
        for k in range(y_t.shape[1] // 128):
            lanes = slice(k * 128, (k + 1) * 128)
            sums[0] += jnp.sum(part[:, :, lanes], axis=0)
            sums[1] += jnp.sum(part[:, :, lanes] * part[:, :, lanes], axis=0)
        y_ref[...] = y_t.astype(BF16).T.reshape(y_ref.shape)

    return [first] + [functools.partial(up, j) for j in range(FF // D)] + [down]


def layer_kernel(pair, pairs, joined, x_ref, near_ref, far_ref, gain_ref, wq_ref, wk_ref, wv_ref, wo_ref, wup_ref, wdn_ref,
                 y_ref, *refs):
    if joined:
        stat_ref = None
    else:
        stat_ref, refs = refs[0], refs[1:]
    layer_steps(pair, pairs, x_ref, near_ref, far_ref, gain_ref, wq_ref, wk_ref, wv_ref, wo_ref, wup_ref, wdn_ref,
                y_ref, stat_ref, *refs)


def layer_steps(pair, pairs, x_ref, near_ref, far_ref, gain_ref, wq_ref, wk_ref, wv_ref, wo_ref, wup_ref, wdn_ref,
                y_ref, stat_ref, wq_t, wv_t, wo_t, wup_t, wdn_t, pos, g1, g2, n1, n2, hidden, sums, *bufs):
    length = pos.shape[1]
    slots = (bufs[0:5], bufs[5:10])
    ctx, scores, weights = bufs[10], bufs[11 : 12 + LEAD], bufs[12 + LEAD :]
    step, last = pl.program_id(0), pairs

    def out_part(sub):
        if stat_ref is not None:
            return pair(y_ref, sub)
        half = y_ref.shape[1] // 2
        return y_ref.at[:, sub * half : (sub + 1) * half]

    def run(sub, a, b, c):
        here, other = slots[sub], slots[1 - sub]
        left, right = [], []
        if c:
            left = pieces_c(here[4], g2[:, :1], wup_t, wdn_t, out_part(sub), sums, n2, hidden)
        if a:
            get = lambda: pair(x_ref, sub)[...].reshape(length, D)
            right = pieces_a(get, pos, g1[:, :1], wq_t, wv_t, wk_ref, *here[:4], n1)
        fills = []
        while left or right:
            fills += left[:1] + right[:1]
            left, right = left[1:], right[1:]
        run_step(fills, (*other, wo_t) if b else None, scores, weights, ctx)

    @pl.when(step == 0)
    def _():
        wq_t[...] = wq_ref[...].T
        wv_t[...] = wv_ref[...].T
        wo_t[...] = wo_ref[...].T
        wup_t[...] = wup_ref[...].T
        wdn_t[...] = wdn_ref[...].T
        g1[...] = jnp.broadcast_to(gain_ref[0:1, :], (128, D)).T
        g2[...] = jnp.broadcast_to(gain_ref[1:2, :], (128, D)).T
        far = far_ref[...].T
        for a in range(length // 128):
            pos[:, a * 128 : (a + 1) * 128] = far[:D, a : a + 1] * near_ref[0] + far[D:, a : a + 1] * near_ref[1]
        for slot in slots:
            slot[3][...] = jnp.ones_like(slot[3])
        sums[...] = jnp.zeros_like(sums)
        run(0, True, False, False)
        run(1, True, True, False)

    @pl.when((step > 0) & (step < last))
    def _():
        run(0, True, True, True)
        run(1, True, True, True)

    @pl.when(step == last)
    def _():
        run(0, False, True, True)
        run(1, False, False, True)
        if stat_ref is not None:
            row = jnp.concatenate([jnp.sum(sums[k], axis=0, keepdims=True) for k in range(2)], axis=1)
            stat_ref[...] = jnp.broadcast_to(row[None], stat_ref.shape)

    if stat_ref is None:
        @pl.when(step == last + 1)
        def _():
            rows = [jnp.sum(sums[k], axis=0, keepdims=True) for k in range(2)]
            terms = [t.astype(F32) for r in rows for t in split_three(r)]
            tile = jnp.concatenate(terms + [jnp.zeros((y_ref.shape[1] - 6, 128), F32)], axis=0)
            tile = jnp.concatenate([tile, jnp.zeros_like(tile)], axis=1).astype(BF16)
            y_ref[...] = jnp.broadcast_to(tile[None], y_ref.shape)


def in_hbm(arrays):
    return [pltpu.with_memory_space_constraint(a, pltpu.HBM) for a in arrays]


def layer(x, count, x_block, x_map, pair, length, level, gain, weights, joined, peers, name):
    near, far = pos_parts(length)
    pick = lambda a: pl.BlockSpec((None, *a.shape[1:]), lambda i: (level,) + (0,) * (a.ndim - 1))
    whole = lambda a: pl.BlockSpec(a.shape, lambda i: (0,) * a.ndim)
    pairs = count // 2
    slot = [
        pltpu.VMEM((D, length), F32), pltpu.VMEM((D, length), BF16), pltpu.VMEM((length, D), BF16),
        pltpu.VMEM((HEADS * AUG, length), BF16), pltpu.VMEM((D, length), F32),
    ]
    if joined is None:
        steps = pairs + 1
        out_specs = [pl.BlockSpec(x_block, lambda i: x_map(jnp.maximum(i - 1, 0))),
                     pl.BlockSpec((peers, 1, 256), lambda i: (0, 0, 0))]
        out_shape = [jax.ShapeDtypeStruct(x.shape, BF16), jax.ShapeDtypeStruct((peers, 1, 256), F32)]
    else:
        steps = pairs + 2
        out_specs = pl.BlockSpec((peers, (joined[1] - 8) // pairs, D), lambda i: (0, jnp.maximum(i - 1, 0), 0))
        out_shape = jax.ShapeDtypeStruct(joined, BF16)
    return pl.pallas_call(
        functools.partial(layer_kernel, pair, pairs, joined is not None),
        grid=(steps,),
        in_specs=[pl.BlockSpec(x_block, lambda i: x_map(jnp.minimum(i, pairs - 1))),
                  whole(near), whole(far), pick(gain)] + [pick(w) for w in weights],
        out_specs=out_specs,
        out_shape=out_shape,
        scratch_shapes=[
            pltpu.VMEM((D, D), BF16), pltpu.VMEM((D, D), BF16), pltpu.VMEM((D, D), BF16),
            pltpu.VMEM((FF, D), BF16), pltpu.VMEM((D, FF), BF16),
            pltpu.VMEM((D, length), F32), pltpu.VMEM((D, 128), F32), pltpu.VMEM((D, 128), F32),
            pltpu.VMEM((D, length), BF16), pltpu.VMEM((D, length), BF16), pltpu.VMEM((FF, length), BF16),
            pltpu.VMEM((2, 8, 128), F32), *slot, *slot, pltpu.VMEM((D, length), BF16),
            *[pltpu.VMEM((length, CHUNK), F32)] * (LEAD + 1), *[pltpu.VMEM((length, CHUNK), BF16)] * (TRAIL + 1),
        ],
        compiler_params=pltpu.CompilerParams(dimension_semantics=("arbitrary",), vmem_limit_bytes=36 << 20),
        name=name,
    )(*(in_hbm if joined is None else tuple)((x, jnp.asarray(near), jnp.asarray(far), gain, *weights)))


def split_three(x):
    high = x.astype(BF16)
    rest = x - high.astype(F32)
    mid = rest.astype(BF16)
    return high, mid, (rest - mid.astype(F32)).astype(BF16)


def affine_of(stat, gain, bias, cells):
    center = stat[0] / cells
    spread = stat[1] / cells - center * center
    slope = gain * lax.rsqrt(spread + EPS)
    return slope, bias - slope * center


def in_vmem(*arrays):
    return [pltpu.with_memory_space_constraint(a, pltpu.VMEM) for a in arrays]


VMEM_SPEC = pl.BlockSpec(memory_space=pltpu.VMEM)


def blend_intra(stat, intra, mixture, gain, bias, cells):
    segs, frames, _ = mixture.shape
    width = 64
    pitch = width + 8

    def kernel(stat_ref, y_ref, x_ref, gain_ref, bias_ref, out_ref, *parts):
        row = jnp.sum(stat_ref[...], axis=0)
        sums = [jnp.sum(row[:, 128 * k : 128 * k + 128], axis=(0, 1), keepdims=True) for k in range(2)]
        slope, offset = affine_of(sums, gain_ref[0:1, :], bias_ref[0:1, :], cells)

        def chunk(i, _):
            at = pl.multiple_of(i * width, width)
            for s in range(segs):
                mixed = slope * y_ref[s, pl.ds(at, width), :].astype(F32) + offset + x_ref[s, pl.ds(at, width), :].astype(F32)
                for k, part in enumerate(parts):
                    part[s * pitch : s * pitch + width, :] = mixed[:, k * 128 : (k + 1) * 128]
            for f in range(width):
                for k, part in enumerate(parts):
                    out_ref[at + f, :, k * 128 : (k + 1) * 128] = part[pl.ds(f, segs, stride=pitch), :].astype(BF16)
            return 0

        lax.fori_loop(0, frames // width, chunk, 0)

    return pl.pallas_call(
        kernel,
        in_specs=[VMEM_SPEC] * 5,
        out_specs=VMEM_SPEC,
        out_shape=jax.ShapeDtypeStruct((frames, segs, D), BF16),
        scratch_shapes=[pltpu.VMEM((segs * pitch, 128), F32)] * 2,
        compiler_params=pltpu.CompilerParams(vmem_limit_bytes=8 << 20),
        name="blend_intra",
    )(*in_vmem(stat, intra, mixture), gain, bias)


def blend_inter(back, across, gain, bias, cells, own):
    frames, segs, _ = across.shape
    peers, rows, _ = back.shape
    width = 64
    pitch, count, steps = segs + 8, width // own, frames // width

    def kernel(back_ref, res_ref, gain_ref, bias_ref, out_ref, stage, sem, *parts):
        tile = jnp.sum(back_ref[:, rows - 8 :, :].astype(F32), axis=0)
        sums = [jnp.sum(tile[3 * k : 3 * k + 3, :], axis=(0, 1), keepdims=True) for k in range(2)]
        slope, offset = affine_of(sums, gain_ref[1:2, :], bias_ref[1:2, :], cells)

        def copy_out(i):
            at = pl.multiple_of(i * width, width)
            return pltpu.make_async_copy(stage.at[i], out_ref.at[:, pl.ds(at, width), :], sem.at[i])

        def chunk(i, _):
            for f in range(width):
                p, j = divmod(f, own)
                data = back_ref[i * count + p, j * segs : (j + 1) * segs, :].astype(F32)
                mixed = slope * data + offset + res_ref[i * width + f].astype(F32)
                for k, part in enumerate(parts):
                    part[f * pitch : f * pitch + segs, :] = mixed[:, k * 128 : (k + 1) * 128]
            for s in range(segs):
                for k, part in enumerate(parts):
                    stage[i, s, :, k * 128 : (k + 1) * 128] = part[pl.ds(s, width, stride=pitch), :].astype(BF16)
            copy_out(i).start()
            return 0

        lax.fori_loop(0, steps, chunk, 0)
        for i in range(steps):
            copy_out(i).wait()

    return pl.pallas_call(
        kernel,
        in_specs=[VMEM_SPEC] * 4,
        out_specs=pl.BlockSpec(memory_space=pl.ANY),
        out_shape=jax.ShapeDtypeStruct((segs, frames, D), BF16),
        scratch_shapes=[pltpu.VMEM((steps, segs, width, D), BF16), pltpu.SemaphoreType.DMA((steps,)),
                        *[pltpu.VMEM((width * pitch, 128), F32)] * 2],
        compiler_params=pltpu.CompilerParams(vmem_limit_bytes=12 << 20),
        name="blend_inter",
    )(*in_vmem(back, across), gain, bias)


def split_three(x):
    high = x.astype(BF16)
    rest = x - high.astype(F32)
    mid = rest.astype(BF16)
    return high, mid, (rest - mid.astype(F32)).astype(BF16)


def body(mixture, w_query, w_key, w_value, w_out, w_up, w_down, ln_gain, gln_gain, gln_bias):
    shards = lax.axis_size("span")
    segs, frames, _ = mixture.shape
    own = frames // shards
    total = segs * shards
    cells = float(total * frames * D)
    weights = (w_query, w_key, w_value, w_out, w_up, w_down)

    intra, stat = layer(mixture, segs, (2, frames, D), lambda i: (i, 0, 0), lambda r, k: r.at[k], frames,
                        0, ln_gain, weights, None, shards, name="intra")
    stat = lax.all_to_all(stat, "span", split_axis=0, concat_axis=0, tiled=True)
    across = blend_intra(stat, intra, mixture, gln_gain, gln_bias, cells)
    moved = lax.all_to_all(across.reshape(shards, own, segs, D), "span", split_axis=0, concat_axis=0, tiled=True)

    rows = own * segs
    inter = layer(moved, own, (shards, 2, segs, D), lambda i: (0, i, 0, 0), lambda r, k: r.at[:, k], total,
                  1, ln_gain, weights, (shards, rows + 8, D), shards, name="inter")
    back = lax.all_to_all(inter, "span", split_axis=0, concat_axis=0, tiled=True)
    return blend_inter(back, across, gln_gain, gln_bias, cells, own)


def solution(mesh):
    in_specs = (P(("mix", "span"), None, None), P(), P(), P(), P(), P(), P(), P(), P(), P())
    out_specs = P(("mix", "span"), None, None)
    return jax.shard_map(body, mesh=mesh, in_specs=in_specs, out_specs=out_specs, check_vma=False)
```

```python
import functools
import math

import jax
import numpy as np
import jax.numpy as jnp
from jax import lax
from jax.experimental import pallas as pl
from jax.experimental.pallas import tpu as pltpu
from jax.sharding import PartitionSpec as P

D = 256
HEADS = 8
HD = D // HEADS
FF = 1024
EPS = 1e-05
AUG = HD + 16
F32 = jnp.float32
BF16 = jnp.bfloat16


def pos_parts(length):
    column = np.arange(D)
    rates = np.exp(-(2 * (column // 2)) / D * math.log(10000.0))[:, None]
    near = np.arange(128)[None, :] * rates
    far = 128 * np.arange(8)[None, :] * rates
    even = (column % 2 == 0)[:, None]
    outer = np.where(even, np.sin(far), np.cos(far))
    swap = np.where(even, np.cos(far), -np.sin(far))
    return (np.stack([np.cos(near), np.sin(near)]).astype(np.float32),
            np.concatenate([outer, swap], axis=0).T.astype(np.float32))


def dot(a, b):
    return lax.dot_general(a, b, (((1,), (0,)), ((), ())), preferred_element_type=F32)


def norm_cols(x, gain):
    center = jnp.mean(x, axis=0, keepdims=True)
    shifted = x - center
    spread = jnp.mean(shifted * shifted, axis=0, keepdims=True)
    return shifted * lax.rsqrt(spread + EPS) * gain


CHUNK = 256
LEAD = 2
TRAIL = 1


def score_unit(q_t, keys, c, h):
    block, at = divmod(h * HD, 128)
    parts = []
    if at:
        parts.append(jnp.zeros((at, CHUNK), BF16))
    parts.append(q_t[h * HD : (h + 1) * HD, c * CHUNK : (c + 1) * CHUNK])
    if at + HD < 128:
        parts.append(jnp.zeros((128 - at - HD, CHUNK), BF16))
    return dot(keys[:, block * 128 : (block + 1) * 128], jnp.concatenate(parts, axis=0))


def run_step(fills, b, scores, weights, ctx):
    if b is None:
        for piece in fills:
            piece()
        return
    x_res, q_t, keys, vaug, after, wo_t = b
    units = [(c, h) for c in range(q_t.shape[1] // CHUNK) for h in range(HEADS)]
    tops = {}
    n = len(units)
    slots = n + LEAD + TRAIL
    done = 0
    for u in range(slots):
        if u < n:
            s = score_unit(q_t, keys, *units[u])
            tops[u] = jnp.max(s, axis=0, keepdims=True)
            scores[u % len(scores)][...] = s
        v = u - LEAD
        if 0 <= v < n:
            s = scores[v % len(scores)][...]
            weights[v % len(weights)][...] = jnp.exp2(s - tops.pop(v)).astype(BF16)
        w = v - TRAIL
        if 0 <= w < n:
            c, h = units[w]
            mixed = dot(vaug[h * AUG : (h + 1) * AUG, :], weights[w % len(weights)][...])
            ctx[h * HD : (h + 1) * HD, c * CHUNK : (c + 1) * CHUNK] = (
                mixed[:HD, :] * (1.0 / mixed[HD : HD + 1, :])
            ).astype(BF16)
        upto = len(fills) * (u + 1) // slots
        for piece in fills[done:upto]:
            piece()
        done = upto
    after[...] = x_res[...] + dot(wo_t[...], ctx[...])


def pieces_a(x, pos, g1, wq_t, wv_t, w_k, x_res, q_t, keys, vaug, n1):
    def first():
        xt = x().T.astype(F32) + pos[...]
        x_res[...] = xt
        n1[...] = norm_cols(xt, g1).astype(BF16)

    def get_keys():
        keys[...] = dot(n1[...].T, w_k[...]).astype(BF16)

    def get_queries():
        scale = math.log2(math.e) / math.sqrt(HD)
        q_t[...] = (dot(wq_t[...], n1[...]) * scale).astype(BF16)

    def get_values():
        v_t = dot(wv_t[...], n1[...]).astype(BF16)
        for h in range(HEADS):
            vaug[h * AUG : h * AUG + HD, :] = v_t[h * HD : (h + 1) * HD, :]

    return [first, get_keys, get_queries, get_values]


def pieces_c(after, g2, wup_t, wdn_t, emit, sums, n2, hidden):
    def first():
        n2[...] = norm_cols(after[...], g2).astype(BF16)

    def up(j):
        rows = slice(j * D, (j + 1) * D)
        hidden[rows, :] = jnp.maximum(dot(wup_t[rows, :], n2[...]), 0.0).astype(BF16)

    def down():
        y_t = after[...] + dot(wdn_t[...], hidden[...])
        part = y_t.reshape(D // 8, 8, y_t.shape[1])
        for k in range(y_t.shape[1] // 128):
            lanes = slice(k * 128, (k + 1) * 128)
            sums[0] += jnp.sum(part[:, :, lanes], axis=0)
            sums[1] += jnp.sum(part[:, :, lanes] * part[:, :, lanes], axis=0)
        emit(y_t.astype(BF16).T)

    return [first] + [functools.partial(up, j) for j in range(FF // D)] + [down]


def layer_steps(pairs, get, emit, finish, near_ref, far_ref, gain_ref, wq_ref, wk_ref, wv_ref, wo_ref, wup_ref, wdn_ref,
                wq_t, wv_t, wo_t, wup_t, wdn_t, pos, g1, g2, n1, n2, hidden, sums, *bufs):
    length = pos.shape[1]
    slots = (bufs[0:5], bufs[5:10])
    ctx, scores, weights = bufs[10], bufs[11 : 12 + LEAD], bufs[12 + LEAD :]
    step, last = pl.program_id(0), pairs

    def run(sub, a, b, c):
        here, other = slots[sub], slots[1 - sub]
        left, right = [], []
        if c:
            left = pieces_c(here[4], g2[:, :1], wup_t, wdn_t, functools.partial(emit, sub), sums, n2, hidden)
        if a:
            right = pieces_a(functools.partial(get, sub), pos, g1[:, :1], wq_t, wv_t, wk_ref, *here[:4], n1)
        fills = []
        while left or right:
            fills += left[:1] + right[:1]
            left, right = left[1:], right[1:]
        run_step(fills, (*other, wo_t) if b else None, scores, weights, ctx)

    @pl.when(step == 0)
    def _():
        wq_t[...] = wq_ref[...].T
        wv_t[...] = wv_ref[...].T
        wo_t[...] = wo_ref[...].T
        wup_t[...] = wup_ref[...].T
        wdn_t[...] = wdn_ref[...].T
        g1[...] = jnp.broadcast_to(gain_ref[0:1, :], (128, D)).T
        g2[...] = jnp.broadcast_to(gain_ref[1:2, :], (128, D)).T
        far = far_ref[...].T
        for a in range(length // 128):
            pos[:, a * 128 : (a + 1) * 128] = far[:D, a : a + 1] * near_ref[0] + far[D:, a : a + 1] * near_ref[1]
        for slot in slots:
            slot[3][...] = jnp.ones_like(slot[3])
        sums[...] = jnp.zeros_like(sums)
        run(0, True, False, False)
        run(1, True, True, False)

    @pl.when((step > 0) & (step < last))
    def _():
        run(0, True, True, True)
        run(1, True, True, True)

    @pl.when(step == last)
    def _():
        run(0, False, True, True)
        run(1, False, False, True)
        finish()


def affine_of(stat, gain, bias, cells):
    center = stat[0] / cells
    spread = stat[1] / cells - center * center
    slope = gain * lax.rsqrt(spread + EPS)
    return slope, bias - slope * center


def in_vmem(*arrays):
    return [pltpu.with_memory_space_constraint(a, pltpu.VMEM) for a in arrays]


VMEM_SPEC = pl.BlockSpec(memory_space=pltpu.VMEM)


def in_hbm(arrays):
    return [pltpu.with_memory_space_constraint(a, pltpu.HBM) for a in arrays]


def split_three(x):
    high = x.astype(BF16)
    rest = x - high.astype(F32)
    mid = rest.astype(BF16)
    return high, mid, (rest - mid.astype(F32)).astype(BF16)


def stat_rows(sums, count):
    terms = [t.astype(F32) for k in range(2) for t in split_three(jnp.sum(sums[k], axis=0, keepdims=True))]
    tile = jnp.concatenate(terms + [jnp.zeros((count - 6, 128), F32)], axis=0)
    return jnp.concatenate([tile, jnp.zeros_like(tile)], axis=1).astype(BF16)


def layer_scratch(length):
    slot = [
        pltpu.VMEM((D, length), F32), pltpu.VMEM((D, length), BF16), pltpu.VMEM((length, D), BF16),
        pltpu.VMEM((HEADS * AUG, length), BF16), pltpu.VMEM((D, length), F32),
    ]
    return [
        pltpu.VMEM((D, D), BF16), pltpu.VMEM((D, D), BF16), pltpu.VMEM((D, D), BF16),
        pltpu.VMEM((FF, D), BF16), pltpu.VMEM((D, FF), BF16),
        pltpu.VMEM((D, length), F32), pltpu.VMEM((D, 128), F32), pltpu.VMEM((D, 128), F32),
        pltpu.VMEM((D, length), BF16), pltpu.VMEM((D, length), BF16), pltpu.VMEM((FF, length), BF16),
        pltpu.VMEM((2, 8, 128), F32), *slot, *slot, pltpu.VMEM((D, length), BF16),
        *[pltpu.VMEM((length, CHUNK), F32)] * (LEAD + 1), *[pltpu.VMEM((length, CHUNK), BF16)] * (TRAIL + 1),
    ]


LAYER_PARAMS = pltpu.CompilerParams(dimension_semantics=("arbitrary",), vmem_limit_bytes=36 << 20)


def intra_layer(mixture, gain, weights, peers):
    segs, frames, _ = mixture.shape
    pairs = segs // 2
    near, far = pos_parts(frames)
    pick = lambda a: pl.BlockSpec((None, *a.shape[1:]), lambda i: (0,) * a.ndim)
    whole = lambda a: pl.BlockSpec(a.shape, lambda i: (0,) * a.ndim)

    def kernel(x_ref, *refs):
        consts, (y_ref, stat_ref), work = refs[:9], refs[9:11], refs[11:]

        def emit(sub, y):
            y_ref[pl.program_id(0) * 2 - 2 + sub] = y

        def finish():
            row = jnp.concatenate([jnp.sum(work[11][k], axis=0, keepdims=True) for k in range(2)], axis=1)
            stat_ref[...] = jnp.broadcast_to(row[None], stat_ref.shape)

        layer_steps(pairs, lambda sub: x_ref[sub], emit, finish, *consts, *work)

    return pl.pallas_call(
        kernel,
        grid=(pairs + 1,),
        in_specs=[pl.BlockSpec((2, frames, D), lambda i: (jnp.minimum(i, pairs - 1), 0, 0)),
                  whole(near), whole(far), pick(gain)] + [pick(w) for w in weights],
        out_specs=[VMEM_SPEC, VMEM_SPEC],
        out_shape=[jax.ShapeDtypeStruct(mixture.shape, BF16), jax.ShapeDtypeStruct((peers, 1, 256), F32)],
        scratch_shapes=layer_scratch(frames),
        compiler_params=LAYER_PARAMS,
        name="intra",
    )(*in_hbm((mixture, jnp.asarray(near), jnp.asarray(far), gain, *weights)))


def inter_layer(moved, gain, weights):
    peers, own, segs, _ = moved.shape
    total, pairs, rows = peers * segs, own // 2, own * segs
    near, far = pos_parts(total)

    def kernel(x_ref, near_ref, far_ref, gain_ref, *refs):
        weights_refs, y_ref, work = [r.at[1] for r in refs[:6]], refs[6], refs[7:]
        step = pl.program_id(0)

        def get(sub):
            return x_ref[:, step * 2 + sub].reshape(total, D)

        def emit(sub, y):
            at = pl.multiple_of((step * 2 - 2 + sub) * segs, segs)
            y_ref[:, pl.ds(at, segs), :] = y.reshape(peers, segs, D)

        def finish():
            y_ref[:, rows:, :] = jnp.broadcast_to(stat_rows(work[11], 8)[None], (peers, 8, D))

        layer_steps(pairs, get, emit, finish, near_ref, far_ref, gain_ref.at[1], *weights_refs, *work)

    return pl.pallas_call(
        kernel,
        grid=(pairs + 1,),
        in_specs=[VMEM_SPEC] * 10,
        out_specs=VMEM_SPEC,
        out_shape=jax.ShapeDtypeStruct((peers, rows + 8, D), BF16),
        scratch_shapes=layer_scratch(total),
        compiler_params=LAYER_PARAMS,
        name="inter",
    )(*in_vmem(moved, jnp.asarray(near), jnp.asarray(far), gain, *weights))


def blend_intra(stat, intra, mixture, gain, bias, cells):
    segs, frames, _ = mixture.shape
    width = 64
    pitch = width + 8

    def kernel(stat_ref, y_ref, x_ref, gain_ref, bias_ref, out_ref, *parts):
        row = jnp.sum(stat_ref[...], axis=0)
        sums = [jnp.sum(row[:, 128 * k : 128 * k + 128], axis=(0, 1), keepdims=True) for k in range(2)]
        slope, offset = affine_of(sums, gain_ref[0:1, :], bias_ref[0:1, :], cells)

        def chunk(i, _):
            at = pl.multiple_of(i * width, width)
            for s in range(segs):
                mixed = slope * y_ref[s, pl.ds(at, width), :].astype(F32) + offset + x_ref[s, pl.ds(at, width), :].astype(F32)
                for k, part in enumerate(parts):
                    part[s * pitch : s * pitch + width, :] = mixed[:, k * 128 : (k + 1) * 128]
            for f in range(width):
                for k, part in enumerate(parts):
                    out_ref[at + f, :, k * 128 : (k + 1) * 128] = part[pl.ds(f, segs, stride=pitch), :].astype(BF16)
            return 0

        lax.fori_loop(0, frames // width, chunk, 0)

    return pl.pallas_call(
        kernel,
        in_specs=[VMEM_SPEC] * 5,
        out_specs=VMEM_SPEC,
        out_shape=jax.ShapeDtypeStruct((frames, segs, D), BF16),
        scratch_shapes=[pltpu.VMEM((segs * pitch, 128), F32)] * 2,
        compiler_params=pltpu.CompilerParams(vmem_limit_bytes=8 << 20),
        name="blend_intra",
    )(*in_vmem(stat, intra, mixture), gain, bias)


def blend_inter(back, across, gain, bias, cells, own):
    frames, segs, _ = across.shape
    peers, rows, _ = back.shape
    width = 64
    pitch, count, steps = segs + 8, width // own, frames // width

    def kernel(back_ref, res_ref, gain_ref, bias_ref, out_ref, stage, sem, *parts):
        tile = jnp.sum(back_ref[:, rows - 8 :, :].astype(F32), axis=0)
        sums = [jnp.sum(tile[3 * k : 3 * k + 3, :], axis=(0, 1), keepdims=True) for k in range(2)]
        slope, offset = affine_of(sums, gain_ref[1:2, :], bias_ref[1:2, :], cells)

        def copy_out(i):
            at = pl.multiple_of(i * width, width)
            return pltpu.make_async_copy(stage.at[i], out_ref.at[:, pl.ds(at, width), :], sem.at[i])

        def chunk(i, _):
            for f in range(width):
                p, j = divmod(f, own)
                data = back_ref[i * count + p, j * segs : (j + 1) * segs, :].astype(F32)
                mixed = slope * data + offset + res_ref[i * width + f].astype(F32)
                for k, part in enumerate(parts):
                    part[f * pitch : f * pitch + segs, :] = mixed[:, k * 128 : (k + 1) * 128]
            for s in range(segs):
                for k, part in enumerate(parts):
                    stage[i, s, :, k * 128 : (k + 1) * 128] = part[pl.ds(s, width, stride=pitch), :].astype(BF16)
            copy_out(i).start()
            return 0

        lax.fori_loop(0, steps, chunk, 0)
        for i in range(steps):
            copy_out(i).wait()

    return pl.pallas_call(
        kernel,
        in_specs=[VMEM_SPEC] * 4,
        out_specs=pl.BlockSpec(memory_space=pl.ANY),
        out_shape=jax.ShapeDtypeStruct((segs, frames, D), BF16),
        scratch_shapes=[pltpu.VMEM((steps, segs, width, D), BF16), pltpu.SemaphoreType.DMA((steps,)),
                        *[pltpu.VMEM((width * pitch, 128), F32)] * 2],
        compiler_params=pltpu.CompilerParams(vmem_limit_bytes=12 << 20),
        name="blend_inter",
    )(*in_vmem(back, across), gain, bias)


def body(mixture, w_query, w_key, w_value, w_out, w_up, w_down, ln_gain, gln_gain, gln_bias):
    shards = lax.axis_size("span")
    segs, frames, _ = mixture.shape
    own = frames // shards
    total = segs * shards
    cells = float(total * frames * D)
    weights = (w_query, w_key, w_value, w_out, w_up, w_down)

    intra, stat = intra_layer(mixture, ln_gain, weights, shards)
    stat = lax.all_to_all(stat, "span", split_axis=0, concat_axis=0, tiled=True)
    across = blend_intra(stat, intra, mixture, gln_gain, gln_bias, cells)
    moved = lax.all_to_all(across.reshape(shards, own, segs, D), "span", split_axis=0, concat_axis=0, tiled=True)

    inter = inter_layer(moved, ln_gain, weights)
    back = lax.all_to_all(inter, "span", split_axis=0, concat_axis=0, tiled=True)
    return blend_inter(back, across, gln_gain, gln_bias, cells, own)


def solution(mesh):
    in_specs = (P(("mix", "span"), None, None), P(), P(), P(), P(), P(), P(), P(), P(), P())
    out_specs = P(("mix", "span"), None, None)
    return jax.shard_map(body, mesh=mesh, in_specs=in_specs, out_specs=out_specs, check_vma=False)
```

```python
import functools
import math

import jax
import numpy as np
import jax.numpy as jnp
from jax import lax
from jax.experimental import pallas as pl
from jax.experimental.pallas import tpu as pltpu
from jax.sharding import PartitionSpec as P

D = 256
HEADS = 8
HD = D // HEADS
FF = 1024
EPS = 1e-05
AUG = HD + 16
F32 = jnp.float32
BF16 = jnp.bfloat16


def pos_parts(length):
    column = np.arange(D)
    rates = np.exp(-(2 * (column // 2)) / D * math.log(10000.0))[:, None]
    near = np.arange(128)[None, :] * rates
    far = 128 * np.arange(8)[None, :] * rates
    even = (column % 2 == 0)[:, None]
    outer = np.where(even, np.sin(far), np.cos(far))
    swap = np.where(even, np.cos(far), -np.sin(far))
    return (np.stack([np.cos(near), np.sin(near)]).astype(np.float32),
            np.concatenate([outer, swap], axis=0).T.astype(np.float32))


def dot(a, b):
    return lax.dot_general(a, b, (((1,), (0,)), ((), ())), preferred_element_type=F32)


def norm_cols(x, gain):
    center = jnp.mean(x, axis=0, keepdims=True)
    shifted = x - center
    spread = jnp.mean(shifted * shifted, axis=0, keepdims=True)
    return shifted * lax.rsqrt(spread + EPS) * gain


INTRA_AHEAD = (4, 2)
INTER_AHEAD = (6, 3)
CHUNK = 256


def score_unit(q_t, keys, c, h):
    block, at = divmod(h * HD, 128)
    parts = []
    if at:
        parts.append(jnp.zeros((at, CHUNK), BF16))
    parts.append(q_t[h * HD : (h + 1) * HD, c * CHUNK : (c + 1) * CHUNK])
    if at + HD < 128:
        parts.append(jnp.zeros((128 - at - HD, CHUNK), BF16))
    return dot(keys[:, block * 128 : (block + 1) * 128], jnp.concatenate(parts, axis=0))


def run_step(fills, b, scores, weights, ctx):
    if b is None:
        for piece in fills:
            piece()
        return
    x_res, q_t, keys, vaug, after, wo_t = b
    units = [(c, h) for c in range(q_t.shape[1] // CHUNK) for h in range(HEADS)]
    tops = {}
    n = len(units)
    lead, trail = len(scores) - 1, len(weights) - 1
    slots = n + lead + trail
    done = 0
    for u in range(slots):
        if u < n:
            s = score_unit(q_t, keys, *units[u])
            tops[u] = jnp.max(s, axis=0, keepdims=True)
            scores[u % len(scores)][...] = s
        v = u - lead
        if 0 <= v < n:
            s = scores[v % len(scores)][...]
            weights[v % len(weights)][...] = jnp.exp2(s - tops.pop(v)).astype(BF16)
        w = v - trail
        if 0 <= w < n:
            c, h = units[w]
            mixed = dot(vaug[h * AUG : (h + 1) * AUG, :], weights[w % len(weights)][...])
            ctx[h * HD : (h + 1) * HD, c * CHUNK : (c + 1) * CHUNK] = (
                mixed[:HD, :] * (1.0 / mixed[HD : HD + 1, :])
            ).astype(BF16)
        upto = len(fills) * (u + 1) // slots
        for piece in fills[done:upto]:
            piece()
        done = upto
    after[...] = x_res[...] + dot(wo_t[...], ctx[...])


def pieces_a(x, pos, g1, wq_t, wv_t, w_k, x_res, q_t, keys, vaug, n1):
    def first():
        xt = x().T.astype(F32) + pos[...]
        x_res[...] = xt
        n1[...] = norm_cols(xt, g1).astype(BF16)

    def get_keys():
        keys[...] = dot(n1[...].T, w_k[...]).astype(BF16)

    def get_queries():
        scale = math.log2(math.e) / math.sqrt(HD)
        q_t[...] = (dot(wq_t[...], n1[...]) * scale).astype(BF16)

    def get_values():
        v_t = dot(wv_t[...], n1[...]).astype(BF16)
        for h in range(HEADS):
            vaug[h * AUG : h * AUG + HD, :] = v_t[h * HD : (h + 1) * HD, :]

    return [first, get_keys, get_queries, get_values]


def pieces_c(after, g2, wup_t, wdn_t, emit, sums, n2, hidden):
    def first():
        n2[...] = norm_cols(after[...], g2).astype(BF16)

    def up(j):
        rows = slice(j * D, (j + 1) * D)
        hidden[rows, :] = jnp.maximum(dot(wup_t[rows, :], n2[...]), 0.0).astype(BF16)

    def down():
        y_t = after[...] + dot(wdn_t[...], hidden[...])
        part = y_t.reshape(D // 8, 8, y_t.shape[1])
        for k in range(y_t.shape[1] // 128):
            lanes = slice(k * 128, (k + 1) * 128)
            sums[0] += jnp.sum(part[:, :, lanes], axis=0)
            sums[1] += jnp.sum(part[:, :, lanes] * part[:, :, lanes], axis=0)
        emit(y_t.astype(BF16).T)

    return [first] + [functools.partial(up, j) for j in range(FF // D)] + [down]


def layer_steps(pairs, lead, get, emit, finish, near_ref, far_ref, gain_ref, wq_ref, wk_ref, wv_ref, wo_ref, wup_ref, wdn_ref,
                wq_t, wv_t, wo_t, wup_t, wdn_t, pos, g1, g2, n1, n2, hidden, sums, *bufs):
    length = pos.shape[1]
    slots = (bufs[0:5], bufs[5:10])
    ctx = bufs[10]
    scores, weights = bufs[11 : 12 + lead], bufs[12 + lead :]
    step, last = pl.program_id(0), pairs

    def run(sub, a, b, c):
        here, other = slots[sub], slots[1 - sub]
        left, right = [], []
        if c:
            left = pieces_c(here[4], g2[:, :1], wup_t, wdn_t, functools.partial(emit, sub), sums, n2, hidden)
        if a:
            right = pieces_a(functools.partial(get, sub), pos, g1[:, :1], wq_t, wv_t, wk_ref, *here[:4], n1)
        fills = []
        while left or right:
            fills += left[:1] + right[:1]
            left, right = left[1:], right[1:]
        run_step(fills, (*other, wo_t) if b else None, scores, weights, ctx)

    @pl.when(step == 0)
    def _():
        wq_t[...] = wq_ref[...].T
        wv_t[...] = wv_ref[...].T
        wo_t[...] = wo_ref[...].T
        wup_t[...] = wup_ref[...].T
        wdn_t[...] = wdn_ref[...].T
        g1[...] = jnp.broadcast_to(gain_ref[0:1, :], (128, D)).T
        g2[...] = jnp.broadcast_to(gain_ref[1:2, :], (128, D)).T
        far = far_ref[...].T
        for a in range(length // 128):
            pos[:, a * 128 : (a + 1) * 128] = far[:D, a : a + 1] * near_ref[0] + far[D:, a : a + 1] * near_ref[1]
        for slot in slots:
            slot[3][...] = jnp.ones_like(slot[3])
        sums[...] = jnp.zeros_like(sums)
        run(0, True, False, False)
        run(1, True, True, False)

    @pl.when((step > 0) & (step < last))
    def _():
        run(0, True, True, True)
        run(1, True, True, True)

    @pl.when(step == last)
    def _():
        run(0, False, True, True)
        run(1, False, False, True)
        finish()


def affine_of(stat, gain, bias, cells):
    center = stat[0] / cells
    spread = stat[1] / cells - center * center
    slope = gain * lax.rsqrt(spread + EPS)
    return slope, bias - slope * center


def in_vmem(*arrays):
    return [pltpu.with_memory_space_constraint(a, pltpu.VMEM) for a in arrays]


VMEM_SPEC = pl.BlockSpec(memory_space=pltpu.VMEM)


def in_hbm(arrays):
    return [pltpu.with_memory_space_constraint(a, pltpu.HBM) for a in arrays]


def split_three(x):
    high = x.astype(BF16)
    rest = x - high.astype(F32)
    mid = rest.astype(BF16)
    return high, mid, (rest - mid.astype(F32)).astype(BF16)


def stat_rows(sums, count):
    terms = [t.astype(F32) for k in range(2) for t in split_three(jnp.sum(sums[k], axis=0, keepdims=True))]
    tile = jnp.concatenate(terms + [jnp.zeros((count - 6, 128), F32)], axis=0)
    return jnp.concatenate([tile, jnp.zeros_like(tile)], axis=1).astype(BF16)


def layer_scratch(length, lead, trail):
    slot = [
        pltpu.VMEM((D, length), F32), pltpu.VMEM((D, length), BF16), pltpu.VMEM((length, D), BF16),
        pltpu.VMEM((HEADS * AUG, length), BF16), pltpu.VMEM((D, length), F32),
    ]
    return [
        pltpu.VMEM((D, D), BF16), pltpu.VMEM((D, D), BF16), pltpu.VMEM((D, D), BF16),
        pltpu.VMEM((FF, D), BF16), pltpu.VMEM((D, FF), BF16),
        pltpu.VMEM((D, length), F32), pltpu.VMEM((D, 128), F32), pltpu.VMEM((D, 128), F32),
        pltpu.VMEM((D, length), BF16), pltpu.VMEM((D, length), BF16), pltpu.VMEM((FF, length), BF16),
        pltpu.VMEM((2, 8, 128), F32), *slot, *slot, pltpu.VMEM((D, length), BF16),
        *[pltpu.VMEM((length, CHUNK), F32)] * (lead + 1), *[pltpu.VMEM((length, CHUNK), BF16)] * (trail + 1),
    ]


LAYER_PARAMS = pltpu.CompilerParams(dimension_semantics=("arbitrary",), vmem_limit_bytes=36 << 20)


def intra_layer(mixture, gain, weights, peers):
    segs, frames, _ = mixture.shape
    pairs = segs // 2
    near, far = pos_parts(frames)
    pick = lambda a: pl.BlockSpec((None, *a.shape[1:]), lambda i: (0,) * a.ndim)
    whole = lambda a: pl.BlockSpec(a.shape, lambda i: (0,) * a.ndim)

    def kernel(x_ref, *refs):
        consts, (y_ref, stat_ref), work = refs[:9], refs[9:11], refs[11:]

        def emit(sub, y):
            y_ref[pl.program_id(0) * 2 - 2 + sub] = y

        def finish():
            row = jnp.concatenate([jnp.sum(work[11][k], axis=0, keepdims=True) for k in range(2)], axis=1)
            stat_ref[...] = jnp.broadcast_to(row[None], stat_ref.shape)

        layer_steps(pairs, INTRA_AHEAD[0], lambda sub: x_ref[sub], emit, finish, *consts, *work)

    return pl.pallas_call(
        kernel,
        grid=(pairs + 1,),
        in_specs=[pl.BlockSpec((2, frames, D), lambda i: (jnp.minimum(i, pairs - 1), 0, 0)),
                  whole(near), whole(far), pick(gain)] + [pick(w) for w in weights],
        out_specs=[VMEM_SPEC, VMEM_SPEC],
        out_shape=[jax.ShapeDtypeStruct(mixture.shape, BF16), jax.ShapeDtypeStruct((peers, 1, 256), F32)],
        scratch_shapes=layer_scratch(frames, *INTRA_AHEAD),
        compiler_params=LAYER_PARAMS,
        name="intra",
    )(*in_hbm((mixture, jnp.asarray(near), jnp.asarray(far), gain, *weights)))


def inter_layer(moved, gain, weights):
    peers, own, segs, _ = moved.shape
    total, pairs, rows = peers * segs, own // 2, own * segs
    near, far = pos_parts(total)

    def kernel(x_ref, near_ref, far_ref, gain_ref, *refs):
        weights_refs, y_ref, work = [r.at[1] for r in refs[:6]], refs[6], refs[7:]
        step = pl.program_id(0)

        def get(sub):
            return x_ref[:, step * 2 + sub].reshape(total, D)

        def emit(sub, y):
            at = pl.multiple_of((step * 2 - 2 + sub) * segs, segs)
            y_ref[:, pl.ds(at, segs), :] = y.reshape(peers, segs, D)

        def finish():
            y_ref[:, rows:, :] = jnp.broadcast_to(stat_rows(work[11], 8)[None], (peers, 8, D))

        layer_steps(pairs, INTER_AHEAD[0], get, emit, finish, near_ref, far_ref, gain_ref.at[1], *weights_refs, *work)

    return pl.pallas_call(
        kernel,
        grid=(pairs + 1,),
        in_specs=[VMEM_SPEC] * 10,
        out_specs=VMEM_SPEC,
        out_shape=jax.ShapeDtypeStruct((peers, rows + 8, D), BF16),
        scratch_shapes=layer_scratch(total, *INTER_AHEAD),
        compiler_params=LAYER_PARAMS,
        name="inter",
    )(*in_vmem(moved, jnp.asarray(near), jnp.asarray(far), gain, *weights))


def blend_intra(stat, intra, mixture, gain, bias, cells):
    segs, frames, _ = mixture.shape
    width = 64
    pitch = width + 8

    def kernel(stat_ref, y_ref, x_ref, gain_ref, bias_ref, out_ref, *parts):
        row = jnp.sum(stat_ref[...], axis=0)
        sums = [jnp.sum(row[:, 128 * k : 128 * k + 128], axis=(0, 1), keepdims=True) for k in range(2)]
        slope, offset = affine_of(sums, gain_ref[0:1, :], bias_ref[0:1, :], cells)

        def chunk(i, _):
            at = pl.multiple_of(i * width, width)
            for s in range(segs):
                mixed = slope * y_ref[s, pl.ds(at, width), :].astype(F32) + offset + x_ref[s, pl.ds(at, width), :].astype(F32)
                for k, part in enumerate(parts):
                    part[s * pitch : s * pitch + width, :] = mixed[:, k * 128 : (k + 1) * 128]
            for f in range(width):
                for k, part in enumerate(parts):
                    out_ref[at + f, :, k * 128 : (k + 1) * 128] = part[pl.ds(f, segs, stride=pitch), :].astype(BF16)
            return 0

        lax.fori_loop(0, frames // width, chunk, 0)

    return pl.pallas_call(
        kernel,
        in_specs=[VMEM_SPEC] * 5,
        out_specs=VMEM_SPEC,
        out_shape=jax.ShapeDtypeStruct((frames, segs, D), BF16),
        scratch_shapes=[pltpu.VMEM((segs * pitch, 128), F32)] * 2,
        compiler_params=pltpu.CompilerParams(vmem_limit_bytes=8 << 20),
        name="blend_intra",
    )(*in_vmem(stat, intra, mixture), gain, bias)


def blend_inter(back, across, gain, bias, cells, own):
    frames, segs, _ = across.shape
    peers, rows, _ = back.shape
    width = 64
    pitch, count, steps = segs + 8, width // own, frames // width

    def kernel(back_ref, res_ref, gain_ref, bias_ref, out_ref, stage, sem, *parts):
        tile = jnp.sum(back_ref[:, rows - 8 :, :].astype(F32), axis=0)
        sums = [jnp.sum(tile[3 * k : 3 * k + 3, :], axis=(0, 1), keepdims=True) for k in range(2)]
        slope, offset = affine_of(sums, gain_ref[1:2, :], bias_ref[1:2, :], cells)

        def copy_out(i):
            at = pl.multiple_of(i * width, width)
            return pltpu.make_async_copy(stage.at[i], out_ref.at[:, pl.ds(at, width), :], sem.at[i])

        def chunk(i, _):
            for f in range(width):
                p, j = divmod(f, own)
                data = back_ref[i * count + p, j * segs : (j + 1) * segs, :].astype(F32)
                mixed = slope * data + offset + res_ref[i * width + f].astype(F32)
                for k, part in enumerate(parts):
                    part[f * pitch : f * pitch + segs, :] = mixed[:, k * 128 : (k + 1) * 128]
            for s in range(segs):
                for k, part in enumerate(parts):
                    stage[i, s, :, k * 128 : (k + 1) * 128] = part[pl.ds(s, width, stride=pitch), :].astype(BF16)
            copy_out(i).start()
            return 0

        lax.fori_loop(0, steps, chunk, 0)
        for i in range(steps):
            copy_out(i).wait()

    return pl.pallas_call(
        kernel,
        in_specs=[VMEM_SPEC] * 4,
        out_specs=pl.BlockSpec(memory_space=pl.ANY),
        out_shape=jax.ShapeDtypeStruct((segs, frames, D), BF16),
        scratch_shapes=[pltpu.VMEM((steps, segs, width, D), BF16), pltpu.SemaphoreType.DMA((steps,)),
                        *[pltpu.VMEM((width * pitch, 128), F32)] * 2],
        compiler_params=pltpu.CompilerParams(vmem_limit_bytes=12 << 20),
        name="blend_inter",
    )(*in_vmem(back, across), gain, bias)


def body(mixture, w_query, w_key, w_value, w_out, w_up, w_down, ln_gain, gln_gain, gln_bias):
    shards = lax.axis_size("span")
    segs, frames, _ = mixture.shape
    own = frames // shards
    total = segs * shards
    cells = float(total * frames * D)
    weights = (w_query, w_key, w_value, w_out, w_up, w_down)

    intra, stat = intra_layer(mixture, ln_gain, weights, shards)
    stat = lax.all_to_all(stat, "span", split_axis=0, concat_axis=0, tiled=True)
    across = blend_intra(stat, intra, mixture, gln_gain, gln_bias, cells)
    moved = lax.all_to_all(across.reshape(shards, own, segs, D), "span", split_axis=0, concat_axis=0, tiled=True)

    inter = inter_layer(moved, ln_gain, weights)
    back = lax.all_to_all(inter, "span", split_axis=0, concat_axis=0, tiled=True)
    return blend_inter(back, across, gln_gain, gln_bias, cells, own)


def solution(mesh):
    in_specs = (P(("mix", "span"), None, None), P(), P(), P(), P(), P(), P(), P(), P(), P())
    out_specs = P(("mix", "span"), None, None)
    return jax.shard_map(body, mesh=mesh, in_specs=in_specs, out_specs=out_specs, check_vma=False)
```

```python
import functools
import math

import jax
import numpy as np
import jax.numpy as jnp
from jax import lax
from jax.experimental import pallas as pl
from jax.experimental.pallas import tpu as pltpu
from jax.sharding import PartitionSpec as P

D = 256
HEADS = 8
HD = D // HEADS
FF = 1024
EPS = 1e-05
AUG = HD + 16
F32 = jnp.float32
BF16 = jnp.bfloat16


def pos_parts(length):
    column = np.arange(D)
    rates = np.exp(-(2 * (column // 2)) / D * math.log(10000.0))[:, None]
    near = np.arange(128)[None, :] * rates
    far = 128 * np.arange(8)[None, :] * rates
    even = (column % 2 == 0)[:, None]
    outer = np.where(even, np.sin(far), np.cos(far))
    swap = np.where(even, np.cos(far), -np.sin(far))
    return (np.stack([np.cos(near), np.sin(near)]).astype(np.float32),
            np.concatenate([outer, swap], axis=0).T.astype(np.float32))


def dot(a, b):
    return lax.dot_general(a, b, (((1,), (0,)), ((), ())), preferred_element_type=F32)


def norm_cols(x, gain):
    center = jnp.mean(x, axis=0, keepdims=True)
    shifted = x - center
    spread = jnp.mean(shifted * shifted, axis=0, keepdims=True)
    return shifted * lax.rsqrt(spread + EPS) * gain


INTRA_AHEAD = (5, 2)
INTER_AHEAD = (7, 3)
CHUNK = 256


def score_unit(q_t, keys, c, h):
    block, at = divmod(h * HD, 128)
    parts = []
    if at:
        parts.append(jnp.zeros((at, CHUNK), BF16))
    parts.append(q_t[h * HD : (h + 1) * HD, c * CHUNK : (c + 1) * CHUNK])
    if at + HD < 128:
        parts.append(jnp.zeros((128 - at - HD, CHUNK), BF16))
    return dot(keys[:, block * 128 : (block + 1) * 128], jnp.concatenate(parts, axis=0))


def run_step(fills, b, scores, weights, ctx):
    if b is None:
        for piece in fills:
            piece()
        return
    x_res, q_t, keys, vaug, after, wo_t = b
    units = [(c, h) for c in range(q_t.shape[1] // CHUNK) for h in range(HEADS)]
    tops = {}
    n = len(units)
    lead, trail = len(scores) - 1, len(weights) - 1
    slots = n + lead + trail
    done = 0
    for u in range(slots):
        if u < n:
            s = score_unit(q_t, keys, *units[u])
            tops[u] = jnp.max(s, axis=0, keepdims=True)
            scores[u % len(scores)][...] = s
        v = u - lead
        if 0 <= v < n:
            s = scores[v % len(scores)][...]
            weights[v % len(weights)][...] = jnp.exp2(s - tops.pop(v)).astype(BF16)
        w = v - trail
        if 0 <= w < n:
            c, h = units[w]
            mixed = dot(vaug[h * AUG : (h + 1) * AUG, :], weights[w % len(weights)][...])
            ctx[h * HD : (h + 1) * HD, c * CHUNK : (c + 1) * CHUNK] = (
                mixed[:HD, :] * (1.0 / mixed[HD : HD + 1, :])
            ).astype(BF16)
        upto = len(fills) * (u + 1) // slots
        for piece in fills[done:upto]:
            piece()
        done = upto
    after[...] = x_res[...] + dot(wo_t[...], ctx[...])


def pieces_a(x, pos, g1, wq_t, wv_t, w_k, x_res, q_t, keys, vaug, n1):
    def first():
        xt = x().T.astype(F32) + pos[...]
        x_res[...] = xt
        n1[...] = norm_cols(xt, g1).astype(BF16)

    def get_keys():
        keys[...] = dot(n1[...].T, w_k[...]).astype(BF16)

    def get_queries():
        scale = math.log2(math.e) / math.sqrt(HD)
        q_t[...] = (dot(wq_t[...], n1[...]) * scale).astype(BF16)

    def get_values():
        v_t = dot(wv_t[...], n1[...]).astype(BF16)
        for h in range(HEADS):
            vaug[h * AUG : h * AUG + HD, :] = v_t[h * HD : (h + 1) * HD, :]

    return [first, get_keys, get_queries, get_values]


def pieces_c(after, g2, wup_t, wdn_t, emit, sums, n2, hidden):
    def first():
        n2[...] = norm_cols(after[...], g2).astype(BF16)

    def up(j):
        rows = slice(j * D, (j + 1) * D)
        hidden[rows, :] = jnp.maximum(dot(wup_t[rows, :], n2[...]).astype(BF16), 0)

    def down():
        y_t = after[...] + dot(wdn_t[...], hidden[...])
        part = y_t.reshape(D // 8, 8, y_t.shape[1])
        for k in range(y_t.shape[1] // 128):
            lanes = slice(k * 128, (k + 1) * 128)
            sums[0] += jnp.sum(part[:, :, lanes], axis=0)
            sums[1] += jnp.sum(part[:, :, lanes] * part[:, :, lanes], axis=0)
        emit(y_t.astype(BF16).T)

    return [first] + [functools.partial(up, j) for j in range(FF // D)] + [down]


def layer_steps(steps, group, lead, get, emit, finish, near_ref, far_ref, gain_ref, wq_ref, wk_ref, wv_ref, wo_ref, wup_ref, wdn_ref,
                wq_t, wv_t, wo_t, wup_t, wdn_t, pos, g1, g2, n1, n2, hidden, sums, *bufs):
    length = pos.shape[1]
    slots = (bufs[0:5], bufs[5:10])
    ctx = bufs[10]
    scores, weights = bufs[11 : 12 + lead], bufs[12 + lead :]
    step, last = pl.program_id(0), steps

    def run(sub, a, b, c):
        here, other = slots[sub % 2], slots[1 - sub % 2]
        left, right = [], []
        if c:
            left = pieces_c(here[4], g2[:, :1], wup_t, wdn_t, functools.partial(emit, sub), sums, n2, hidden)
        if a:
            right = pieces_a(functools.partial(get, sub), pos, g1[:, :1], wq_t, wv_t, wk_ref, *here[:4], n1)
        fills = []
        while left or right:
            fills += left[:1] + right[:1]
            left, right = left[1:], right[1:]
        run_step(fills, (*other, wo_t) if b else None, scores, weights, ctx)

    @pl.when(step == 0)
    def _():
        wq_t[...] = wq_ref[...].T
        wv_t[...] = wv_ref[...].T
        wo_t[...] = wo_ref[...].T
        wup_t[...] = wup_ref[...].T
        wdn_t[...] = wdn_ref[...].T
        g1[...] = jnp.broadcast_to(gain_ref[0:1, :], (128, D)).T
        g2[...] = jnp.broadcast_to(gain_ref[1:2, :], (128, D)).T
        far = far_ref[...].T
        for a in range(length // 128):
            pos[:, a * 128 : (a + 1) * 128] = far[:D, a : a + 1] * near_ref[0] + far[D:, a : a + 1] * near_ref[1]
        for slot in slots:
            slot[3][...] = jnp.ones_like(slot[3])
        sums[...] = jnp.zeros_like(sums)
        for sub in range(group):
            run(sub, True, sub >= 1, sub >= 2)

    @pl.when((step > 0) & (step < last))
    def _():
        for sub in range(group):
            run(sub, True, True, True)

    @pl.when(step == last)
    def _():
        run(0, False, True, True)
        run(1, False, False, True)
        finish()


def affine_of(stat, gain, bias, cells):
    center = stat[0] / cells
    spread = stat[1] / cells - center * center
    slope = gain * lax.rsqrt(spread + EPS)
    return slope, bias - slope * center


def in_vmem(*arrays):
    return [pltpu.with_memory_space_constraint(a, pltpu.VMEM) for a in arrays]


VMEM_SPEC = pl.BlockSpec(memory_space=pltpu.VMEM)


def in_hbm(arrays):
    return [pltpu.with_memory_space_constraint(a, pltpu.HBM) for a in arrays]


def split_three(x):
    high = x.astype(BF16)
    rest = x - high.astype(F32)
    mid = rest.astype(BF16)
    return high, mid, (rest - mid.astype(F32)).astype(BF16)


def stat_rows(sums, count):
    terms = [t.astype(F32) for k in range(2) for t in split_three(jnp.sum(sums[k], axis=0, keepdims=True))]
    tile = jnp.concatenate(terms + [jnp.zeros((count - 6, 128), F32)], axis=0)
    return jnp.concatenate([tile, jnp.zeros_like(tile)], axis=1).astype(BF16)


def layer_scratch(length, lead, trail):
    slot = [
        pltpu.VMEM((D, length), F32), pltpu.VMEM((D, length), BF16), pltpu.VMEM((length, D), BF16),
        pltpu.VMEM((HEADS * AUG, length), BF16), pltpu.VMEM((D, length), F32),
    ]
    return [
        pltpu.VMEM((D, D), BF16), pltpu.VMEM((D, D), BF16), pltpu.VMEM((D, D), BF16),
        pltpu.VMEM((FF, D), BF16), pltpu.VMEM((D, FF), BF16),
        pltpu.VMEM((D, length), F32), pltpu.VMEM((D, 128), F32), pltpu.VMEM((D, 128), F32),
        pltpu.VMEM((D, length), BF16), pltpu.VMEM((D, length), BF16), pltpu.VMEM((FF, length), BF16),
        pltpu.VMEM((2, 8, 128), F32), *slot, *slot, pltpu.VMEM((D, length), BF16),
        *[pltpu.VMEM((length, CHUNK), F32)] * (lead + 1), *[pltpu.VMEM((length, CHUNK), BF16)] * (trail + 1),
    ]


LAYER_PARAMS = pltpu.CompilerParams(dimension_semantics=("arbitrary",), vmem_limit_bytes=36 << 20)


def intra_layer(mixture, gain, weights, peers):
    segs, frames, _ = mixture.shape
    group = 4
    near, far = pos_parts(frames)
    pick = lambda a: pl.BlockSpec((None, *a.shape[1:]), lambda i: (0,) * a.ndim)
    whole = lambda a: pl.BlockSpec(a.shape, lambda i: (0,) * a.ndim)

    def kernel(x_ref, *refs):
        consts, (y_ref, stat_ref), work = refs[:9], refs[9:11], refs[11:]

        def emit(sub, y):
            y_ref[pl.program_id(0) * group - 2 + sub] = y

        def finish():
            row = jnp.concatenate([jnp.sum(work[11][k], axis=0, keepdims=True) for k in range(2)], axis=1)
            stat_ref[...] = jnp.broadcast_to(row[None], stat_ref.shape)

        layer_steps(segs // group, group, INTRA_AHEAD[0], lambda sub: x_ref[sub], emit, finish, *consts, *work)

    return pl.pallas_call(
        kernel,
        grid=(segs // group + 1,),
        in_specs=[pl.BlockSpec((group, frames, D), lambda i: (jnp.minimum(i, segs // group - 1), 0, 0)),
                  whole(near), whole(far), pick(gain)] + [pick(w) for w in weights],
        out_specs=[VMEM_SPEC, VMEM_SPEC],
        out_shape=[jax.ShapeDtypeStruct(mixture.shape, BF16), jax.ShapeDtypeStruct((peers, 1, 256), F32)],
        scratch_shapes=layer_scratch(frames, *INTRA_AHEAD),
        compiler_params=LAYER_PARAMS,
        name="intra",
    )(*in_hbm((mixture, jnp.asarray(near), jnp.asarray(far), gain, *weights)))


def inter_layer(moved, gain, weights):
    peers, own, segs, _ = moved.shape
    total, pairs, rows = peers * segs, own // 2, own * segs
    near, far = pos_parts(total)

    def kernel(x_ref, near_ref, far_ref, gain_ref, *refs):
        weights_refs, y_ref, work = [r.at[1] for r in refs[:6]], refs[6], refs[7:]
        step = pl.program_id(0)

        def get(sub):
            return x_ref[:, step * 2 + sub].reshape(total, D)

        def emit(sub, y):
            at = pl.multiple_of((step * 2 - 2 + sub) * segs, segs)
            y_ref[:, pl.ds(at, segs), :] = y.reshape(peers, segs, D)

        def finish():
            y_ref[:, rows:, :] = jnp.broadcast_to(stat_rows(work[11], 8)[None], (peers, 8, D))

        layer_steps(pairs, 2, INTER_AHEAD[0], get, emit, finish, near_ref, far_ref, gain_ref.at[1], *weights_refs, *work)

    return pl.pallas_call(
        kernel,
        grid=(pairs + 1,),
        in_specs=[VMEM_SPEC] * 10,
        out_specs=VMEM_SPEC,
        out_shape=jax.ShapeDtypeStruct((peers, rows + 8, D), BF16),
        scratch_shapes=layer_scratch(total, *INTER_AHEAD),
        compiler_params=LAYER_PARAMS,
        name="inter",
    )(*in_vmem(moved, jnp.asarray(near), jnp.asarray(far), gain, *weights))


def blend_intra(stat, intra, mixture, gain, bias, cells):
    segs, frames, _ = mixture.shape
    width = 64
    pitch = width + 8

    def kernel(stat_ref, y_ref, x_ref, gain_ref, bias_ref, out_ref, *parts):
        row = jnp.sum(stat_ref[...], axis=0)
        sums = [jnp.sum(row[:, 128 * k : 128 * k + 128], axis=(0, 1), keepdims=True) for k in range(2)]
        slope, offset = affine_of(sums, gain_ref[0:1, :], bias_ref[0:1, :], cells)

        def chunk(i, _):
            at = pl.multiple_of(i * width, width)
            for s in range(segs):
                mixed = slope * y_ref[s, pl.ds(at, width), :].astype(F32) + offset + x_ref[s, pl.ds(at, width), :].astype(F32)
                for k, part in enumerate(parts):
                    part[s * pitch : s * pitch + width, :] = mixed[:, k * 128 : (k + 1) * 128]
            for f in range(width):
                for k, part in enumerate(parts):
                    out_ref[at + f, :, k * 128 : (k + 1) * 128] = part[pl.ds(f, segs, stride=pitch), :].astype(BF16)
            return 0

        lax.fori_loop(0, frames // width, chunk, 0)

    return pl.pallas_call(
        kernel,
        in_specs=[VMEM_SPEC] * 5,
        out_specs=VMEM_SPEC,
        out_shape=jax.ShapeDtypeStruct((frames, segs, D), BF16),
        scratch_shapes=[pltpu.VMEM((segs * pitch, 128), F32)] * 2,
        compiler_params=pltpu.CompilerParams(vmem_limit_bytes=8 << 20),
        name="blend_intra",
    )(*in_vmem(stat, intra, mixture), gain, bias)


def blend_inter(back, across, gain, bias, cells, own):
    frames, segs, _ = across.shape
    peers, rows, _ = back.shape
    width = 64
    pitch, count, steps = segs + 8, width // own, frames // width

    def kernel(back_ref, res_ref, gain_ref, bias_ref, out_ref, stage, sem, *parts):
        tile = jnp.sum(back_ref[:, rows - 8 :, :].astype(F32), axis=0)
        sums = [jnp.sum(tile[3 * k : 3 * k + 3, :], axis=(0, 1), keepdims=True) for k in range(2)]
        slope, offset = affine_of(sums, gain_ref[1:2, :], bias_ref[1:2, :], cells)

        def copy_out(i):
            at = pl.multiple_of(i * width, width)
            return pltpu.make_async_copy(stage.at[i], out_ref.at[:, pl.ds(at, width), :], sem.at[i])

        def chunk(i, _):
            for f in range(width):
                p, j = divmod(f, own)
                data = back_ref[i * count + p, j * segs : (j + 1) * segs, :].astype(F32)
                mixed = slope * data + offset + res_ref[i * width + f].astype(F32)
                for k, part in enumerate(parts):
                    part[f * pitch : f * pitch + segs, :] = mixed[:, k * 128 : (k + 1) * 128]
            for s in range(segs):
                for k, part in enumerate(parts):
                    stage[i, s, :, k * 128 : (k + 1) * 128] = part[pl.ds(s, width, stride=pitch), :].astype(BF16)
            copy_out(i).start()
            return 0

        lax.fori_loop(0, steps, chunk, 0)
        for i in range(steps):
            copy_out(i).wait()

    return pl.pallas_call(
        kernel,
        in_specs=[VMEM_SPEC] * 4,
        out_specs=pl.BlockSpec(memory_space=pl.ANY),
        out_shape=jax.ShapeDtypeStruct((segs, frames, D), BF16),
        scratch_shapes=[pltpu.VMEM((steps, segs, width, D), BF16), pltpu.SemaphoreType.DMA((steps,)),
                        *[pltpu.VMEM((width * pitch, 128), F32)] * 2],
        compiler_params=pltpu.CompilerParams(vmem_limit_bytes=12 << 20),
        name="blend_inter",
    )(*in_vmem(back, across), gain, bias)


def body(mixture, w_query, w_key, w_value, w_out, w_up, w_down, ln_gain, gln_gain, gln_bias):
    shards = lax.axis_size("span")
    segs, frames, _ = mixture.shape
    own = frames // shards
    total = segs * shards
    cells = float(total * frames * D)
    weights = (w_query, w_key, w_value, w_out, w_up, w_down)

    intra, stat = intra_layer(mixture, ln_gain, weights, shards)
    stat = lax.all_to_all(stat, "span", split_axis=0, concat_axis=0, tiled=True)
    across = blend_intra(stat, intra, mixture, gln_gain, gln_bias, cells)
    moved = lax.all_to_all(across.reshape(shards, own, segs, D), "span", split_axis=0, concat_axis=0, tiled=True)

    inter = inter_layer(moved, ln_gain, weights)
    back = lax.all_to_all(inter, "span", split_axis=0, concat_axis=0, tiled=True)
    return blend_inter(back, across, gln_gain, gln_bias, cells, own)


def solution(mesh):
    in_specs = (P(("mix", "span"), None, None), P(), P(), P(), P(), P(), P(), P(), P(), P())
    out_specs = P(("mix", "span"), None, None)
    return jax.shard_map(body, mesh=mesh, in_specs=in_specs, out_specs=out_specs, check_vma=False)
```

```python
import functools
import math

import jax
import numpy as np
import jax.numpy as jnp
from jax import lax
from jax.experimental import pallas as pl
from jax.experimental.pallas import tpu as pltpu
from jax.sharding import PartitionSpec as P

D = 256
HEADS = 8
HD = D // HEADS
FF = 1024
EPS = 1e-05
AUG = HD + 16
F32 = jnp.float32
BF16 = jnp.bfloat16


def pos_parts(length):
    column = np.arange(D)
    rates = np.exp(-(2 * (column // 2)) / D * math.log(10000.0))[:, None]
    near = np.arange(128)[None, :] * rates
    far = 128 * np.arange(8)[None, :] * rates
    even = (column % 2 == 0)[:, None]
    outer = np.where(even, np.sin(far), np.cos(far))
    swap = np.where(even, np.cos(far), -np.sin(far))
    return (np.stack([np.cos(near), np.sin(near)]).astype(np.float32),
            np.concatenate([outer, swap], axis=0).T.astype(np.float32))


def dot(a, b):
    return lax.dot_general(a, b, (((1,), (0,)), ((), ())), preferred_element_type=F32)


def norm_cols(x, gain):
    center = jnp.mean(x, axis=0, keepdims=True)
    shifted = x - center
    spread = jnp.mean(shifted * shifted, axis=0, keepdims=True)
    return shifted * lax.rsqrt(spread + EPS) * gain


INTRA_AHEAD = (5, 2)
INTER_AHEAD = (7, 3)
CHUNK = 256


def score_unit(q_t, keys, c, h):
    block, at = divmod(h * HD, 128)
    parts = []
    if at:
        parts.append(jnp.zeros((at, CHUNK), BF16))
    parts.append(q_t[h * HD : (h + 1) * HD, c * CHUNK : (c + 1) * CHUNK])
    if at + HD < 128:
        parts.append(jnp.zeros((128 - at - HD, CHUNK), BF16))
    return dot(keys[:, block * 128 : (block + 1) * 128], jnp.concatenate(parts, axis=0))


def run_step(fills, b, scores, weights, ctx):
    if b is None:
        for piece in fills:
            piece()
        return
    x_res, q_t, keys, vaug, after, wo_t = b
    units = [(c, h) for c in range(q_t.shape[1] // CHUNK) for h in range(HEADS)]
    tops = {}
    n = len(units)
    lead, trail = len(scores) - 1, len(weights) - 1
    slots = n + lead + trail
    done = 0
    for u in range(slots):
        if u < n:
            s = score_unit(q_t, keys, *units[u])
            tops[u] = jnp.max(s, axis=0, keepdims=True)
            scores[u % len(scores)][...] = s
        v = u - lead
        if 0 <= v < n:
            s = scores[v % len(scores)][...]
            weights[v % len(weights)][...] = jnp.exp2(s - tops.pop(v)).astype(BF16)
        w = v - trail
        if 0 <= w < n:
            c, h = units[w]
            mixed = dot(vaug[h * AUG : (h + 1) * AUG, :], weights[w % len(weights)][...])
            ctx[h * HD : (h + 1) * HD, c * CHUNK : (c + 1) * CHUNK] = (
                mixed[:HD, :] * (1.0 / mixed[HD : HD + 1, :])
            ).astype(BF16)
        upto = len(fills) * (u + 1) // slots
        for piece in fills[done:upto]:
            piece()
        done = upto
    after[...] = x_res[...] + dot(wo_t[...], ctx[...])


def pieces_a(x, pos, g1, wq_t, wv_t, w_k, x_res, q_t, keys, vaug, n1):
    def first():
        xt = x().T.astype(F32) + pos[...]
        x_res[...] = xt
        n1[...] = norm_cols(xt, g1).astype(BF16)

    def get_keys():
        keys[...] = dot(n1[...].T, w_k[...]).astype(BF16)

    def get_queries():
        scale = math.log2(math.e) / math.sqrt(HD)
        q_t[...] = (dot(wq_t[...], n1[...]) * scale).astype(BF16)

    def get_values():
        v_t = dot(wv_t[...], n1[...]).astype(BF16)
        for h in range(HEADS):
            vaug[h * AUG : h * AUG + HD, :] = v_t[h * HD : (h + 1) * HD, :]

    return [first, get_keys, get_queries, get_values]


def pieces_c(after, g2, wup_t, wdn_t, emit, sums, n2, hidden):
    def first():
        n2[...] = norm_cols(after[...], g2).astype(BF16)

    def up(j):
        rows = slice(j * D, (j + 1) * D)
        hidden[rows, :] = jnp.maximum(dot(wup_t[rows, :], n2[...]).astype(BF16), 0)

    def down():
        y_t = after[...] + dot(wdn_t[...], hidden[...])
        part = y_t.reshape(D // 8, 8, y_t.shape[1])
        for k in range(y_t.shape[1] // 128):
            lanes = slice(k * 128, (k + 1) * 128)
            sums[0] += jnp.sum(part[:, :, lanes], axis=0)
            sums[1] += jnp.sum(part[:, :, lanes] * part[:, :, lanes], axis=0)
        emit(y_t.astype(BF16).T)

    return [first] + [functools.partial(up, j) for j in range(FF // D)] + [down]


def layer_steps(steps, group, lead, get, emit, finish, near_ref, far_ref, gain_ref, wq_ref, wk_ref, wv_ref, wo_ref, wup_ref, wdn_ref,
                wq_t, wv_t, wo_t, wup_t, wdn_t, pos, g1, g2, n1, n2, hidden, sums, *bufs):
    length = pos.shape[1]
    slots = (bufs[0:5], bufs[5:10])
    ctx = bufs[10]
    scores, weights = bufs[11 : 12 + lead], bufs[12 + lead :]
    step, last = pl.program_id(0), steps

    def run(sub, a, b, c):
        here, other = slots[sub % 2], slots[1 - sub % 2]
        left, right = [], []
        if c:
            left = pieces_c(here[4], g2[:, :1], wup_t, wdn_t, functools.partial(emit, sub), sums, n2, hidden)
        if a:
            right = pieces_a(functools.partial(get, sub), pos, g1[:, :1], wq_t, wv_t, wk_ref, *here[:4], n1)
        fills = []
        while left or right:
            fills += left[:1] + right[:1]
            left, right = left[1:], right[1:]
        run_step(fills, (*other, wo_t) if b else None, scores, weights, ctx)

    @pl.when(step == 0)
    def _():
        wq_t[...] = wq_ref[...].T
        wv_t[...] = wv_ref[...].T
        wo_t[...] = wo_ref[...].T
        wup_t[...] = wup_ref[...].T
        wdn_t[...] = wdn_ref[...].T
        g1[...] = jnp.broadcast_to(gain_ref[0:1, :], (128, D)).T
        g2[...] = jnp.broadcast_to(gain_ref[1:2, :], (128, D)).T
        far = far_ref[...].T
        for a in range(length // 128):
            pos[:, a * 128 : (a + 1) * 128] = far[:D, a : a + 1] * near_ref[0] + far[D:, a : a + 1] * near_ref[1]
        for slot in slots:
            slot[3][...] = jnp.ones_like(slot[3])
        sums[...] = jnp.zeros_like(sums)
        for sub in range(group):
            run(sub, True, sub >= 1, sub >= 2)

    @pl.when((step > 0) & (step < last))
    def _():
        for sub in range(group):
            run(sub, True, True, True)

    @pl.when(step == last)
    def _():
        run(0, False, True, True)
        run(1, False, False, True)
        finish()


def affine_of(stat, gain, bias, cells):
    center = stat[0] / cells
    spread = stat[1] / cells - center * center
    slope = gain * lax.rsqrt(spread + EPS)
    return slope, bias - slope * center


def in_vmem(*arrays):
    return [pltpu.with_memory_space_constraint(a, pltpu.VMEM) for a in arrays]


VMEM_SPEC = pl.BlockSpec(memory_space=pltpu.VMEM)


def in_hbm(arrays):
    return [pltpu.with_memory_space_constraint(a, pltpu.HBM) for a in arrays]


def split_three(x):
    high = x.astype(BF16)
    rest = x - high.astype(F32)
    mid = rest.astype(BF16)
    return high, mid, (rest - mid.astype(F32)).astype(BF16)


def stat_rows(sums, count):
    terms = [t.astype(F32) for k in range(2) for t in split_three(jnp.sum(sums[k], axis=0, keepdims=True))]
    tile = jnp.concatenate(terms + [jnp.zeros((count - 6, 128), F32)], axis=0)
    return jnp.concatenate([tile, jnp.zeros_like(tile)], axis=1).astype(BF16)


def layer_scratch(length, lead, trail):
    slot = [
        pltpu.VMEM((D, length), F32), pltpu.VMEM((D, length), BF16), pltpu.VMEM((length, D), BF16),
        pltpu.VMEM((HEADS * AUG, length), BF16), pltpu.VMEM((D, length), F32),
    ]
    return [
        pltpu.VMEM((D, D), BF16), pltpu.VMEM((D, D), BF16), pltpu.VMEM((D, D), BF16),
        pltpu.VMEM((FF, D), BF16), pltpu.VMEM((D, FF), BF16),
        pltpu.VMEM((D, length), F32), pltpu.VMEM((D, 128), F32), pltpu.VMEM((D, 128), F32),
        pltpu.VMEM((D, length), BF16), pltpu.VMEM((D, length), BF16), pltpu.VMEM((FF, length), BF16),
        pltpu.VMEM((2, 8, 128), F32), *slot, *slot, pltpu.VMEM((D, length), BF16),
        *[pltpu.VMEM((length, CHUNK), F32)] * (lead + 1), *[pltpu.VMEM((length, CHUNK), BF16)] * (trail + 1),
    ]


LAYER_PARAMS = pltpu.CompilerParams(dimension_semantics=("arbitrary",), vmem_limit_bytes=36 << 20)


def intra_layer(mixture, gain, weights, peers):
    segs, frames, _ = mixture.shape
    group = 4
    near, far = pos_parts(frames)
    pick = lambda a: pl.BlockSpec((None, *a.shape[1:]), lambda i: (0,) * a.ndim)
    whole = lambda a: pl.BlockSpec(a.shape, lambda i: (0,) * a.ndim)

    def kernel(x_ref, *refs):
        consts, (y_ref, stat_ref), work = refs[:9], refs[9:11], refs[11:]

        def emit(sub, y):
            y_ref[pl.program_id(0) * group - 2 + sub] = y

        def finish():
            row = jnp.concatenate([jnp.sum(work[11][k], axis=0, keepdims=True) for k in range(2)], axis=1)
            stat_ref[...] = jnp.broadcast_to(row[None], stat_ref.shape)

        layer_steps(segs // group, group, INTRA_AHEAD[0], lambda sub: x_ref[sub], emit, finish, *consts, *work)

    return pl.pallas_call(
        kernel,
        grid=(segs // group + 1,),
        in_specs=[pl.BlockSpec((group, frames, D), lambda i: (jnp.minimum(i, segs // group - 1), 0, 0)),
                  whole(near), whole(far), pick(gain)] + [pick(w) for w in weights],
        out_specs=[VMEM_SPEC, VMEM_SPEC],
        out_shape=[jax.ShapeDtypeStruct(mixture.shape, BF16), jax.ShapeDtypeStruct((peers, 1, 256), F32)],
        scratch_shapes=layer_scratch(frames, *INTRA_AHEAD),
        compiler_params=LAYER_PARAMS,
        name="intra",
    )(*in_hbm((mixture, jnp.asarray(near), jnp.asarray(far), gain, *weights)))


def inter_layer(moved, gain, weights):
    peers, own, segs, _ = moved.shape
    total, pairs, rows = peers * segs, own // 2, own * segs
    near, far = pos_parts(total)

    def kernel(x_ref, near_ref, far_ref, gain_ref, *refs):
        weights_refs, y_ref, work = [r.at[1] for r in refs[:6]], refs[6], refs[7:]
        step = pl.program_id(0)

        def get(sub):
            return x_ref[:, step * 2 + sub].reshape(total, D)

        def emit(sub, y):
            at = pl.multiple_of((step * 2 - 2 + sub) * segs, segs)
            y_ref[:, pl.ds(at, segs), :] = y.reshape(peers, segs, D)

        def finish():
            y_ref[:, rows:, :] = jnp.broadcast_to(stat_rows(work[11], 8)[None], (peers, 8, D))

        layer_steps(pairs, 2, INTER_AHEAD[0], get, emit, finish, near_ref, far_ref, gain_ref.at[1], *weights_refs, *work)

    return pl.pallas_call(
        kernel,
        grid=(pairs + 1,),
        in_specs=[VMEM_SPEC] * 10,
        out_specs=VMEM_SPEC,
        out_shape=jax.ShapeDtypeStruct((peers, rows + 8, D), BF16),
        scratch_shapes=layer_scratch(total, *INTER_AHEAD),
        compiler_params=LAYER_PARAMS,
        name="inter",
    )(*in_vmem(moved, jnp.asarray(near), jnp.asarray(far), gain, *weights))


def blend_intra(stat, intra, mixture, gain, bias, cells):
    segs, frames, _ = mixture.shape
    width = 64
    pitch = width + 8

    def kernel(stat_ref, y_ref, x_ref, gain_ref, bias_ref, out_ref, *parts):
        row = jnp.sum(stat_ref[...], axis=0)
        sums = [jnp.sum(row[:, 128 * k : 128 * k + 128], axis=(0, 1), keepdims=True) for k in range(2)]
        slope, offset = affine_of(sums, gain_ref[0:1, :], bias_ref[0:1, :], cells)

        def chunk(i, _):
            at = pl.multiple_of(i * width, width)
            for s in range(segs):
                mixed = slope * y_ref[s, pl.ds(at, width), :].astype(F32) + offset + x_ref[s, pl.ds(at, width), :].astype(F32)
                for k, part in enumerate(parts):
                    part[s * pitch : s * pitch + width, :] = mixed[:, k * 128 : (k + 1) * 128]
            for f in range(width):
                for k, part in enumerate(parts):
                    out_ref[at + f, :, k * 128 : (k + 1) * 128] = part[pl.ds(f, segs, stride=pitch), :].astype(BF16)
            return 0

        lax.fori_loop(0, frames // width, chunk, 0)

    return pl.pallas_call(
        kernel,
        in_specs=[VMEM_SPEC] * 5,
        out_specs=VMEM_SPEC,
        out_shape=jax.ShapeDtypeStruct((frames, segs, D), BF16),
        scratch_shapes=[pltpu.VMEM((segs * pitch, 128), F32)] * 2,
        compiler_params=pltpu.CompilerParams(vmem_limit_bytes=8 << 20),
        name="blend_intra",
    )(*in_vmem(stat, intra, mixture), gain, bias)


def blend_inter(back, across, gain, bias, cells, own):
    frames, segs, _ = across.shape
    peers, rows, _ = back.shape
    width = 32
    pitch, count, steps = segs + 8, width // own, frames // width

    def kernel(back_ref, res_ref, gain_ref, bias_ref, out_ref, stage, sem, *parts):
        tile = jnp.sum(back_ref[:, rows - 8 :, :].astype(F32), axis=0)
        sums = [jnp.sum(tile[3 * k : 3 * k + 3, :], axis=(0, 1), keepdims=True) for k in range(2)]
        slope, offset = affine_of(sums, gain_ref[1:2, :], bias_ref[1:2, :], cells)

        def copy_out(i):
            at = pl.multiple_of(i * width, width)
            return pltpu.make_async_copy(stage.at[i], out_ref.at[:, pl.ds(at, width), :], sem.at[i])

        def chunk(i, _):
            for f in range(width):
                p, j = divmod(f, own)
                data = back_ref[i * count + p, j * segs : (j + 1) * segs, :].astype(F32)
                mixed = slope * data + offset + res_ref[i * width + f].astype(F32)
                for k, part in enumerate(parts):
                    part[f * pitch : f * pitch + segs, :] = mixed[:, k * 128 : (k + 1) * 128]
            for s in range(segs):
                for k, part in enumerate(parts):
                    stage[i, s, :, k * 128 : (k + 1) * 128] = part[pl.ds(s, width, stride=pitch), :].astype(BF16)
            copy_out(i).start()
            return 0

        lax.fori_loop(0, steps, chunk, 0)
        for i in range(steps):
            copy_out(i).wait()

    return pl.pallas_call(
        kernel,
        in_specs=[VMEM_SPEC] * 4,
        out_specs=pl.BlockSpec(memory_space=pl.ANY),
        out_shape=jax.ShapeDtypeStruct((segs, frames, D), BF16),
        scratch_shapes=[pltpu.VMEM((steps, segs, width, D), BF16), pltpu.SemaphoreType.DMA((steps,)),
                        *[pltpu.VMEM((width * pitch, 128), F32)] * 2],
        compiler_params=pltpu.CompilerParams(vmem_limit_bytes=12 << 20),
        name="blend_inter",
    )(*in_vmem(back, across), gain, bias)


def body(mixture, w_query, w_key, w_value, w_out, w_up, w_down, ln_gain, gln_gain, gln_bias):
    shards = lax.axis_size("span")
    segs, frames, _ = mixture.shape
    own = frames // shards
    total = segs * shards
    cells = float(total * frames * D)
    weights = (w_query, w_key, w_value, w_out, w_up, w_down)

    intra, stat = intra_layer(mixture, ln_gain, weights, shards)
    stat = lax.all_to_all(stat, "span", split_axis=0, concat_axis=0, tiled=True)
    across = blend_intra(stat, intra, mixture, gln_gain, gln_bias, cells)
    moved = lax.all_to_all(across.reshape(shards, own, segs, D), "span", split_axis=0, concat_axis=0, tiled=True)

    inter = inter_layer(moved, ln_gain, weights)
    back = lax.all_to_all(inter, "span", split_axis=0, concat_axis=0, tiled=True)
    return blend_inter(back, across, gln_gain, gln_bias, cells, own)


def solution(mesh):
    in_specs = (P(("mix", "span"), None, None), P(), P(), P(), P(), P(), P(), P(), P(), P())
    out_specs = P(("mix", "span"), None, None)
    return jax.shard_map(body, mesh=mesh, in_specs=in_specs, out_specs=out_specs, check_vma=False)
```
